16 devices in a mesh: dp: 2 (over z), tp: 8 (over y, x, core).
Axes of the slice: x: 2, y: 2, z: 2, core: 2. Of those that a mesh axis runs over, the one named last changes fastest.
Arguments:
- hidden: bfloat16 [1024, 2560], P('dp'), parts along dimension 0
- norm_gain: float32 [2560], replicated
- emb_table: bfloat16 [32768, 2560], P('tp')
- teacher_ids: int32 [1024, 256], P('dp'), parts along dimension 0
- teacher_q: float32 [1024, 256], P('dp'), parts along dimension 0
Outputs:
- output 1: float32 [2], P('dp'), parts along dimension 0
- output 2: bfloat16 [1024, 2560], P('dp'), parts along dimension 0
- output 3: float32 [5120], P('dp'), parts along dimension 0
- output 4: float32 [65536, 2560], P(('dp', 'tp')), parts along dimension 0
There are 2 independent parts. The reference program is written for one: setup_inputs(seed, part) draws one part's arguments, and reference() takes and returns one part's arrays. A program takes and returns all parts, laid end to end along the dimension named above; an argument that names none is the same for every part.
All inputs are finite; a program needn't handle non-finite values.
Results may differ from the reference program's by a relative error of at most 0.001.
Values sent between devices are 32-bit elements.
A program may use at most 1 GiB of HBM per device.

```python
import math
import jax
import jax.numpy as jnp
from jax import lax

TOKENS = 512
VOCAB = 32768
D = 2560
TEACHER_K = 256


def norm_apply(hid_f, gain_vec):
    inv_rms = lax.rsqrt(jnp.mean(hid_f * hid_f, axis=-1, keepdims=True) + 1e-6)
    return hid_f * inv_rms * (1.0 + gain_vec)


def draw_ids(key_ids):
    hot_count = TEACHER_K - TEACHER_K // 2
    cold_count = TEACHER_K // 2
    stride = (VOCAB - 2 * hot_count) // cold_count
    key_bit, key_jit, key_perm = jax.random.split(key_ids, 3)
    hot_ids = 2 * jnp.arange(hot_count)[None, :] + jax.random.randint(key_bit, (TOKENS, hot_count), 0, 2)
    cold_ids = 2 * hot_count + stride * jnp.arange(cold_count)[None, :] + jax.random.randint(key_jit, (TOKENS, cold_count), 0, stride)
    hot_ids = hot_ids.at[0].set(2 * jnp.arange(hot_count))
    cold_ids = cold_ids.at[0].set(2 * hot_count + stride * jnp.arange(cold_count) + stride - 1)
    all_ids = jnp.concatenate([hot_ids, cold_ids], axis=1)
    column_order = jax.random.permutation(key_perm, TEACHER_K)
    return all_ids[:, column_order].astype(jnp.int32)


def setup_inputs(seed: int = 0, part: int = 0) -> dict:
    root_key = jax.random.key(seed)
    key_tab, key_gain, key_dir = jax.random.split(root_key, 3)
    part_key = jax.random.fold_in(jax.random.key(seed + 1), part)
    key_hid, key_ids, key_wts = jax.random.split(part_key, 3)
    direction = jax.random.normal(key_dir, (D,), jnp.float32)
    direction = direction / jnp.sqrt(jnp.sum(direction * direction))
    spread = math.sqrt(0.5 * math.log(VOCAB) / D)
    offset = 24.0 / math.sqrt(D)
    emb_table = spread * jax.random.normal(key_tab, (VOCAB, D), jnp.float32) + offset * direction[None, :]
    norm_gain = 0.3 * jax.random.normal(key_gain, (D,), jnp.float32)
    hidden = jax.random.normal(key_hid, (TOKENS, D), jnp.float32) + 1.5 * math.sqrt(D) * direction[None, :]
    teacher_ids = draw_ids(key_ids)
    hot_mask = (teacher_ids < 2 * (TEACHER_K - TEACHER_K // 2)).astype(jnp.float32)
    scores = 0.8 * jax.random.normal(key_wts, (TOKENS, TEACHER_K), jnp.float32) + 0.5 * hot_mask
    teacher_q = jax.nn.softmax(scores, axis=-1)
    return {'hidden': hidden.astype(jnp.bfloat16), 'norm_gain': norm_gain, 'emb_table': emb_table.astype(jnp.bfloat16), 'teacher_ids': teacher_ids, 'teacher_q': teacher_q}


def reference(hidden, norm_gain, emb_table, teacher_ids, teacher_q):
    normed, norm_pull = jax.vjp(norm_apply, hidden.astype(jnp.float32), norm_gain)
    x_in = normed.astype(jnp.bfloat16)
    logits = jnp.dot(x_in, emb_table.T, preferred_element_type=jnp.float32)
    row_peak = jnp.max(logits, axis=1, keepdims=True)
    log_z = row_peak[:, 0] + jnp.log(jnp.sum(jnp.exp(logits - row_peak), axis=1))
    picked = jnp.take_along_axis(logits, teacher_ids, axis=1)
    q_total = jnp.sum(teacher_q, axis=1)
    token_loss = q_total * log_z - jnp.sum(teacher_q * picked, axis=1)
    mean_loss = jnp.mean(token_loss)[None]
    softmax_p = jnp.exp(logits - log_z[:, None])
    row_index = jnp.arange(TOKENS)[:, None]
    target_q = jnp.zeros((TOKENS, VOCAB), jnp.float32).at[row_index, teacher_ids].add(teacher_q)
    grad_z = ((softmax_p * q_total[:, None] - target_q) / TOKENS).astype(jnp.bfloat16)
    grad_x = jnp.dot(grad_z, emb_table, preferred_element_type=jnp.float32)
    grad_table = jnp.dot(grad_z.T, x_in, preferred_element_type=jnp.float32)
    grad_h, grad_gain = norm_pull(grad_x)
    return (mean_loss, grad_h.astype(jnp.bfloat16), grad_gain, grad_table)
```

```python
import jax
import jax.numpy as jnp
from jax import lax
from jax.experimental import pallas as pl
from jax.experimental.pallas import tpu as pltpu
from jax.sharding import PartitionSpec as P

MESH = pl.DeviceIdType.MESH
F32 = jnp.float32
BF16 = jnp.bfloat16
NT = (((1,), (1,)), ((), ()))
TN = (((0,), (0,)), ((), ()))
CHUNKS = 4
VT = 256


def fused_kernel(n_dev, h_hbm, w_ref, e_hbm, ids_hbm, q_hbm,
                 dh_hbm, dw_ref, loss_ref, dz_hbm, x_hbm,
                 h_v, x_v, e_v, ids_v, q_v, z_v, mx_v, sm_v, lz_v, sn_v, qs_v, dz_v, dx_v, dh_v, g_v,
                 r0_v, r1_v, r2_v, st_send, st_recv, fin_send, fin_recv, dwacc_v, qz_v,
                 e_sem, in_sem, out_sem, st_ss, st_rs, fin_ss, fin_rs, ss, rs):
    tokens, dim = h_v.shape
    vocab = e_v.shape[0]
    rows_c = tokens // CHUNKS
    groups = vocab // 128
    half = rows_c // 2
    n_blk = vocab // VT
    me = lax.axis_index('tp')
    dp = lax.axis_index('dp')
    core = me % 2
    xc = (me // 2) % 2
    yc = me // 4
    sib = me + 1 - 2 * core
    xn = me + 2 - 4 * xc
    yn = me + 4 - 8 * yc
    base = me * vocab
    inv_tokens = 1.0 / tokens

    def al(value, mult):
        return pl.multiple_of(value, mult)

    h_copy = pltpu.make_async_copy(h_hbm, h_v, in_sem.at[0])
    h_copy.start()

    def e_copy(i):
        rows = pl.ds(al(i * VT, VT), VT)
        return pltpu.make_async_copy(e_hbm.at[rows], e_v.at[rows], e_sem.at[i])

    @pl.loop(0, n_blk)
    def _(i):
        e_copy(i).start()

    ids_copy = pltpu.make_async_copy(ids_hbm, ids_v, in_sem.at[1])
    q_copy = pltpu.make_async_copy(q_hbm, q_v, in_sem.at[2])
    ids_copy.start()
    q_copy.start()

    barrier = pltpu.get_barrier_semaphore()
    for i in range(1, n_dev):
        pl.semaphore_signal(barrier, inc=1, device_id=(dp, (me + i) % n_dev), device_id_type=MESH)

    h_copy.wait()
    gain = w_ref[...] + 1.0

    @pl.loop(0, tokens // 16)
    def _(i):
        rows = pl.ds(al(i * 16, 16), 16)
        hf = h_v[rows, :].astype(F32)
        inv = lax.rsqrt(jnp.mean(hf * hf, axis=1, keepdims=True) + 1e-6)
        x_v[rows, :] = (hf * inv * gain).astype(BF16)

    x_copy = pltpu.make_async_copy(x_v, x_hbm, out_sem.at[0])
    x_copy.start()

    mx_v[...] = jnp.full(mx_v.shape, -jnp.inf, F32)

    @pl.loop(0, n_blk)
    def _(i):
        e_copy(i).wait()
        zb = lax.dot_general(x_v[...], e_v[pl.ds(al(i * VT, VT), VT), :], NT, preferred_element_type=F32)
        z_v[:, pl.ds(al(i * VT, VT), VT)] = zb
        top = zb[:, 0:128]
        for k in range(1, VT // 128):
            top = jnp.maximum(top, zb[:, 128 * k:128 * (k + 1)])
        mx_v[...] = jnp.maximum(mx_v[...], top)

    @pl.loop(0, tokens // 32)
    def _(i):
        rows = pl.ds(al(i * 32, 32), 32)
        peak = jnp.max(mx_v[rows, :], axis=1, keepdims=True)
        acc = jnp.zeros((32, 128), F32)
        for k in range(groups):
            acc = acc + jnp.exp(z_v[rows, 128 * k:128 * (k + 1)] - peak)
        mx_v[rows, :] = jnp.broadcast_to(peak, (32, 128))
        sm_v[rows, :] = jnp.broadcast_to(jnp.sum(acc, axis=1, keepdims=True), (32, 128))

    for b in range(tokens // 128):
        span = slice(128 * b, 128 * (b + 1))
        st_send[:, 128 * b:128 * (b + 1)] = mx_v[span, :].T[0:1, :]
        st_send[:, tokens + 128 * b:tokens + 128 * (b + 1)] = sm_v[span, :].T[0:1, :]
    st_recv[me] = st_send[...]

    pl.semaphore_wait(barrier, n_dev - 1)

    def gather_copies(src, dst, s_sem, r_sem):
        out = []
        for i in range(1, n_dev):
            out.append(pltpu.make_async_remote_copy(
                src_ref=src, dst_ref=dst.at[me], send_sem=s_sem.at[i - 1], recv_sem=r_sem.at[i - 1],
                device_id=(dp, (me + i) % n_dev), device_id_type=MESH))
        return out

    st_copies = gather_copies(st_send, st_recv, st_ss, st_rs)
    for copy in st_copies:
        copy.start()

    ids_copy.wait()
    q_copy.wait()

    iota_hi = lax.broadcasted_iota(jnp.int32, (groups, 256), 0)
    iota_lo = lax.broadcasted_iota(jnp.int32, (128, 256), 0)

    def build_q(c):
        @pl.loop(0, rows_c // 8)
        def _(t):
            for u in range(8):
                local = t * 8 + u
                row = pl.ds(c * rows_c + local, 1)
                ids = ids_v[row, :] - base
                qv = q_v[row, :]
                q_a = qv.astype(BF16).astype(F32)
                rest = qv - q_a
                q_b = rest.astype(BF16).astype(F32)
                q_c = rest - q_b
                hot_hi = lax.shift_right_arithmetic(ids, 7) == iota_hi
                hot_lo = jnp.where((ids & 127) == iota_lo, 1.0, 0.0).astype(BF16)
                parts = [jnp.where(hot_hi, part, 0.0).astype(BF16) for part in (q_a, q_b, q_c)]
                res = lax.dot_general(jnp.concatenate(parts, axis=0), hot_lo, NT, preferred_element_type=F32)
                dense = res[0:groups] + res[groups:2 * groups] + res[2 * groups:3 * groups]
                qs_v[pl.ds(local, groups, stride=rows_c), :] = dense

    def make_dz(c):
        @pl.loop(0, rows_c // 16)
        def _(i):
            off = al(i * 16, 16)
            rows = pl.ds(al(c * rows_c + off, 16), 16)
            lz = lz_v[rows, :]
            sn = sn_v[rows, :]
            acc = jnp.zeros((16, 128), F32)
            for k in range(groups):
                zz = z_v[rows, 128 * k:128 * (k + 1)]
                qq = qs_v[pl.ds(al(k * rows_c + off, 16), 16), :]
                acc = acc + qq * zz
                d = (jnp.exp(zz - lz) * sn - qq) * inv_tokens
                dz_v[rows, 128 * k:128 * (k + 1)] = d.astype(BF16)
            qz_v[...] = qz_v[...] + acc

    def make_dx(c):
        rows = slice(c * rows_c, (c + 1) * rows_c)

        @pl.loop(0, dim // 256)
        def _(j):
            cols = pl.ds(al(j * 256, 256), 256)
            dx_v[rows, cols] = jnp.dot(dz_v[rows, :], e_v[:, cols], preferred_element_type=F32)

    q8 = half // 8
    q4 = half // 4
    q2 = half // 2

    def rcopy(src, dst, c, slot, dev):
        return pltpu.make_async_remote_copy(
            src_ref=src, dst_ref=dst, send_sem=ss.at[c, slot], recv_sem=rs.at[c, slot],
            device_id=(dp, dev), device_id_type=MESH)

    def mine(c):
        return c * rows_c + half * core

    sent = []

    def go(*copies):
        for copy in copies:
            copy.start()
            sent.append(copy)

    def s0(c):
        return rcopy(dx_v.at[pl.ds(al(c * rows_c + half * (1 - core), half), half)], r0_v.at[c], c, 0, sib)

    def s1(c):
        a = rcopy(dx_v.at[pl.ds(al(mine(c) + q4 * (1 - xc), q4), q4)], r1_v.at[c, 0], c, 1, xn)
        b = rcopy(dx_v.at[pl.ds(al(mine(c) + q2 + q4 * (1 - yc), q4), q4)], r1_v.at[c, 1], c, 2, yn)
        return a, b

    def s2(c):
        a = rcopy(dx_v.at[pl.ds(al(mine(c) + q4 * xc + q8 * (1 - yc), q8), q8)], r2_v.at[c, 0], c, 3, yn)
        b = rcopy(dx_v.at[pl.ds(al(mine(c) + q2 + q4 * yc + q8 * (1 - xc), q8), q8)], r2_v.at[c, 1], c, 4, xn)
        return a, b

    def s3(c):
        rows_a = pl.ds(al(mine(c) + q4 * xc + q8 * yc, q8), q8)
        rows_b = pl.ds(al(mine(c) + q2 + q4 * yc + q8 * xc, q8), q8)
        return (rcopy(g_v.at[rows_a], g_v.at[rows_a], c, 5, yn), rcopy(g_v.at[rows_b], g_v.at[rows_b], c, 6, xn))

    def s4(c):
        rows_a = pl.ds(al(mine(c) + q4 * xc, q4), q4)
        rows_b = pl.ds(al(mine(c) + q2 + q4 * yc, q4), q4)
        return (rcopy(g_v.at[rows_a], g_v.at[rows_a], c, 7, xn), rcopy(g_v.at[rows_b], g_v.at[rows_b], c, 8, yn))

    def s5(c):
        rows = pl.ds(al(mine(c), half), half)
        return rcopy(g_v.at[rows], g_v.at[rows], c, 9, sib)

    def f0(c):
        go(s0(c))

    def f1(c):
        s0(c).wait_recv()

        @pl.loop(0, half // 8)
        def _(i):
            rows = pl.ds(al(mine(c) + 8 * i, 8), 8)
            dx_v[rows, :] = dx_v[rows, :] + r0_v[c, pl.ds(al(8 * i, 8), 8), :]
        go(*s1(c))

    def f2(c):
        a, b = s1(c)
        a.wait_recv()
        b.wait_recv()
        for k, start in ((0, mine(c) + q4 * xc), (1, mine(c) + q2 + q4 * yc)):
            rows = pl.ds(al(start, q4), q4)
            dx_v[rows, :] = dx_v[rows, :] + r1_v[c, k]
        go(*s2(c))

    def norm_back(c, k, block, side):
        rows16 = pl.ds(al(block, 16), 16)
        rows = pl.ds(al(block + q8 * side, q8), q8)
        hb = h_v[rows16, :].astype(F32)
        hf = jnp.where(side == 0, hb[0:8, :], hb[8:16, :])
        grad = dx_v[rows, :] + r2_v[c, k]
        inv = lax.rsqrt(jnp.mean(hf * hf, axis=1, keepdims=True) + 1e-6)
        scaled = grad * gain
        mean = jnp.sum(scaled * hf, axis=1, keepdims=True) * (1.0 / dim)
        g_v[rows, :] = scaled * inv - hf * (inv * inv * inv * mean)
        dwacc_v[...] = dwacc_v[...] + grad * hf * inv

    def f3(c):
        a, b = s2(c)
        a.wait_recv()
        b.wait_recv()
        norm_back(c, 0, mine(c) + q4 * xc, yc)
        norm_back(c, 1, mine(c) + q2 + q4 * yc, xc)
        go(*s3(c))

    def f4(c):
        a, b = s3(c)
        a.wait_recv()
        b.wait_recv()
        go(*s4(c))

    def f5(c):
        a, b = s4(c)
        a.wait_recv()
        b.wait_recv()
        go(s5(c))

    def rows_of(c):
        return slice(c * rows_c, (c + 1) * rows_c)

    def dh_copy(c):
        return pltpu.make_async_copy(dh_v.at[rows_of(c)], dh_hbm.at[rows_of(c)], out_sem.at[1 + c])

    def dz_copy(c):
        return pltpu.make_async_copy(dz_v.at[rows_of(c)], dz_hbm.at[rows_of(c)], out_sem.at[1 + CHUNKS + c])

    def f6(c):
        s5(c).wait_recv()

        @pl.loop(0, rows_c // 16)
        def _(i):
            rows = pl.ds(al(c * rows_c + 16 * i, 16), 16)
            dh_v[rows, :] = g_v[rows, :].astype(BF16)
        dh_copy(c).start()

    dwacc_v[...] = jnp.zeros(dwacc_v.shape, F32)
    qz_v[...] = jnp.zeros(qz_v.shape, F32)
    build_q(0)

    @pl.loop(0, tokens // 16)
    def _(i):
        rows = pl.ds(al(i * 16, 16), 16)
        sn_v[rows, :] = jnp.broadcast_to(jnp.sum(q_v[rows, :], axis=1, keepdims=True), (16, 128))

    for copy in st_copies:
        copy.wait_recv()
    peak = st_recv[0][:, 0:tokens]
    for d in range(1, n_dev):
        peak = jnp.maximum(peak, st_recv[d][:, 0:tokens])
    total = jnp.zeros((1, tokens), F32)
    for d in range(n_dev):
        total = total + st_recv[d][:, tokens:2 * tokens] * jnp.exp(st_recv[d][:, 0:tokens] - peak)
    log_z = peak + jnp.log(total)
    for b in range(tokens // 128):
        lz_v[128 * b:128 * (b + 1), :] = jnp.broadcast_to(log_z[:, 128 * b:128 * (b + 1)], (128, 128)).T

    def chunk(c):
        make_dz(c)
        dz_copy(c).start()
        make_dx(c)

    chunk(0)
    f0(0)
    build_q(1)
    f1(0)
    chunk(1)
    f0(1)
    f2(0)
    build_q(2)
    f1(1)
    f3(0)
    chunk(2)
    f0(2)
    f2(1)
    f4(0)
    build_q(3)
    f1(2)
    f3(1)
    f5(0)
    chunk(3)
    f0(3)
    f2(2)
    f4(1)
    f6(0)
    f1(3)
    f3(2)
    f5(1)
    f2(3)
    f4(2)
    f6(1)
    f3(3)
    fin_send[:, 0:dim] = jnp.sum(dwacc_v[...], axis=0, keepdims=True)
    fin_send[:, dim:dim + 128] = jnp.sum(qz_v[...], axis=0, keepdims=True)
    fin_recv[me] = fin_send[...]
    fin_copies = gather_copies(fin_send, fin_recv, fin_ss, fin_rs)
    for copy in fin_copies:
        copy.start()
    f5(2)
    f4(3)
    f6(2)
    f5(3)

    for copy in fin_copies:
        copy.wait_recv()
    fin = fin_recv[0]
    for d in range(1, n_dev):
        fin = fin + fin_recv[d]
    dw_ref[...] = fin[:, 0:dim]
    weighted = jnp.sum(lz_v[...] * sn_v[...], axis=0, keepdims=True)
    loss_ref[...] = (weighted - jnp.sum(fin[:, dim:dim + 128])) * inv_tokens
    f6(3)

    for copy in st_copies + sent + fin_copies:
        copy.wait_send()
    x_copy.wait()
    for c in range(CHUNKS):
        dz_copy(c).wait()
        dh_copy(c).wait()


def table_kernel(dz_ref, x_ref, out_ref):
    out_ref[...] = lax.dot_general(dz_ref[...], x_ref[...], TN, preferred_element_type=F32)


def solution(mesh):
    n_dev = mesh.shape['tp']

    def local_step(hidden, norm_gain, emb_block, teacher_ids, teacher_q):
        tokens, dim = hidden.shape
        vocab = emb_block.shape[0]
        rows_c = tokens // CHUNKS
        half = rows_c // 2
        kt = teacher_ids.shape[1]
        any_spec = pl.BlockSpec(memory_space=pl.ANY)
        vmem_spec = pl.BlockSpec(memory_space=pltpu.VMEM)
        vm = pltpu.VMEM
        dma = pltpu.SemaphoreType.DMA
        dh, dw, loss, dz, x_in = pl.pallas_call(
            lambda *refs: fused_kernel(n_dev, *refs),
            out_shape=(
                jax.ShapeDtypeStruct((tokens, dim), BF16),
                jax.ShapeDtypeStruct((1, dim), F32),
                jax.ShapeDtypeStruct((1, 128), F32),
                jax.ShapeDtypeStruct((tokens, vocab), BF16),
                jax.ShapeDtypeStruct((tokens, dim), BF16),
            ),
            in_specs=[any_spec, vmem_spec, any_spec, any_spec, any_spec],
            out_specs=(any_spec, vmem_spec, vmem_spec, any_spec, any_spec),
            scratch_shapes=[
                vm((tokens, dim), BF16),
                vm((tokens, dim), BF16),
                vm((vocab, dim), BF16),
                vm((tokens, kt), jnp.int32),
                vm((tokens, kt), F32),
                vm((tokens, vocab), F32),
                vm((tokens, 128), F32),
                vm((tokens, 128), F32),
                vm((tokens, 128), F32),
                vm((tokens, 128), F32),
                vm((vocab // 128 * rows_c, 128), F32),
                vm((tokens, vocab), BF16),
                vm((tokens, dim), F32),
                vm((tokens, dim), BF16),
                vm((tokens, dim), F32),
                vm((CHUNKS, half, dim), F32),
                vm((CHUNKS, 2, half // 4, dim), F32),
                vm((CHUNKS, 2, half // 8, dim), F32),
                vm((1, 2 * tokens), F32),
                vm((n_dev, 1, 2 * tokens), F32),
                vm((1, dim + 128), F32),
                vm((n_dev, 1, dim + 128), F32),
                vm((8, dim), F32),
                vm((16, 128), F32),
                dma((vocab // VT,)),
                dma((3,)),
                dma((1 + 2 * CHUNKS,)),
                dma((n_dev - 1,)),
                dma((n_dev - 1,)),
                dma((n_dev - 1,)),
                dma((n_dev - 1,)),
                dma((CHUNKS, 10)),
                dma((CHUNKS, 10)),
            ],
            compiler_params=pltpu.CompilerParams(
                collective_id=0, has_side_effects=True, vmem_limit_bytes=67_043_328),
            name='fused_head',
        )(hidden, norm_gain[None, :], emb_block, teacher_ids, teacher_q)
        grad_block = pl.pallas_call(
            table_kernel,
            grid=(vocab // VT,),
            in_specs=[pl.BlockSpec((tokens, VT), lambda i: (0, i)), pl.BlockSpec((tokens, dim), lambda i: (0, 0))],
            out_specs=pl.BlockSpec((VT, dim), lambda i: (i, 0)),
            out_shape=jax.ShapeDtypeStruct((vocab, dim), F32),
            name='table_grad',
        )(dz, x_in)
        return (loss[0, 0:1], dh, dw[0], grad_block)

    return jax.shard_map(local_step, mesh=mesh, in_specs=(P('dp', None), P(None), P('tp', None), P('dp', None), P('dp', None)), out_specs=(P('dp'), P('dp', None), P('dp'), P(('dp', 'tp'), None)), check_vma=False)
```

```python
import jax
import jax.numpy as jnp
from jax import lax
from jax.experimental import pallas as pl
from jax.experimental.pallas import tpu as pltpu
from jax.sharding import PartitionSpec as P

MESH = pl.DeviceIdType.MESH
F32 = jnp.float32
BF16 = jnp.bfloat16
NT = (((1,), (1,)), ((), ()))
TN = (((0,), (0,)), ((), ()))
CHUNKS = 4
VT = 256
SLOTS = 4


def fused_kernel(n_dev, h_hbm, w_ref, e_hbm, ids_hbm, q_hbm,
                 dh_hbm, dw_ref, loss_ref, dz_hbm, x_hbm,
                 h_v, x_v, e_v, ids_v, q_v, z_v, mx_v, sm_v, lz_v, sn_v, qs_v, dz_v, dx_v, dh_v, g_v,
                 r0_v, r1_v, r2_v, st_send, st_recv, fin_send, fin_recv, dwacc_v, qz_v,
                 e_sem, in_sem, out_sem, st_ss, st_rs, fin_ss, fin_rs, ss, rs):
    tokens, dim = h_v.shape
    vocab = e_v.shape[0]
    rows_c = tokens // CHUNKS
    groups = vocab // 128
    half = rows_c // 2
    n_blk = vocab // VT
    me = lax.axis_index('tp')
    dp = lax.axis_index('dp')
    core = me % 2
    xc = (me // 2) % 2
    yc = me // 4
    sib = me + 1 - 2 * core
    xn = me + 2 - 4 * xc
    yn = me + 4 - 8 * yc
    base = me * vocab
    inv_tokens = 1.0 / tokens

    def al(value, mult):
        return pl.multiple_of(value, mult)

    h_copy = pltpu.make_async_copy(h_hbm, h_v, in_sem.at[0])
    ids_copy = pltpu.make_async_copy(ids_hbm, ids_v, in_sem.at[1])
    q_copy = pltpu.make_async_copy(q_hbm, q_v, in_sem.at[2])
    q_copy.start()
    h_copy.start()

    def e_copy(i):
        rows = pl.ds(al(i * VT, VT), VT)
        return pltpu.make_async_copy(e_hbm.at[rows], e_v.at[rows], e_sem.at[i])

    @pl.loop(0, n_blk)
    def _(i):
        e_copy(i).start()

    ids_copy.start()

    barrier = pltpu.get_barrier_semaphore()
    for i in range(1, n_dev):
        pl.semaphore_signal(barrier, inc=1, device_id=(dp, (me + i) % n_dev), device_id_type=MESH)

    q_copy.wait()

    @pl.loop(0, tokens // 64)
    def _(i):
        rows = pl.ds(al(i * 64, 64), 64)
        sn_v[rows, :] = jnp.broadcast_to(jnp.sum(q_v[rows, :], axis=1, keepdims=True), (64, 128))

    h_copy.wait()
    gain = w_ref[...].reshape(1, dim) + 1.0

    @pl.loop(0, tokens // 64)
    def _(i):
        rows = pl.ds(al(i * 64, 64), 64)
        acc = jnp.zeros((64, 128), F32)
        for k in range(dim // 128):
            hf = h_v[rows, 128 * k:128 * (k + 1)].astype(F32)
            acc = acc + hf * hf
        inv = lax.rsqrt(jnp.sum(acc, axis=1, keepdims=True) * (1.0 / dim) + 1e-6)
        inv = jnp.broadcast_to(inv, (64, 128))
        for k in range(dim // 128):
            hf = h_v[rows, 128 * k:128 * (k + 1)].astype(F32)
            x_v[rows, 128 * k:128 * (k + 1)] = (hf * inv * gain[:, 128 * k:128 * (k + 1)]).astype(BF16)

    x_copy = pltpu.make_async_copy(x_v, x_hbm, out_sem.at[0])
    x_copy.start()

    mx_v[...] = jnp.full(mx_v.shape, -jnp.inf, F32)
    sm_v[...] = jnp.zeros(sm_v.shape, F32)

    @pl.loop(0, n_blk)
    def _(i):
        e_copy(i).wait()
        zb = lax.dot_general(x_v[...], e_v[pl.ds(al(i * VT, VT), VT), :], NT, preferred_element_type=F32)
        z_v[:, pl.ds(al(i * VT, VT), VT)] = zb
        old = mx_v[...]
        new = old
        for k in range(VT // 128):
            new = jnp.maximum(new, zb[:, 128 * k:128 * (k + 1)])
        total = sm_v[...] * jnp.exp(old - new)
        for k in range(VT // 128):
            total = total + jnp.exp(zb[:, 128 * k:128 * (k + 1)] - new)
        mx_v[...] = new
        sm_v[...] = total

    for b in range(tokens // 128):
        span = slice(128 * b, 128 * (b + 1))
        peaks = mx_v[span, :].T
        peak = jnp.max(peaks, axis=0, keepdims=True)
        st_send[:, 128 * b:128 * (b + 1)] = peak
        st_send[:, tokens + 128 * b:tokens + 128 * (b + 1)] = jnp.sum(
            sm_v[span, :].T * jnp.exp(peaks - peak), axis=0, keepdims=True)
    st_recv[me] = st_send[...]

    pl.semaphore_wait(barrier, n_dev - 1)

    def gather_copies(src, dst, s_sem, r_sem):
        out = []
        for i in range(1, n_dev):
            out.append(pltpu.make_async_remote_copy(
                src_ref=src, dst_ref=dst.at[me], send_sem=s_sem.at[i - 1], recv_sem=r_sem.at[i - 1],
                device_id=(dp, (me + i) % n_dev), device_id_type=MESH))
        return out

    st_copies = gather_copies(st_send, st_recv, st_ss, st_rs)
    for copy in st_copies:
        copy.start()

    ids_copy.wait()

    iota_hi = lax.broadcasted_iota(jnp.int32, (groups, 256), 0)
    iota_lo = lax.broadcasted_iota(jnp.int32, (128, 256), 0)

    def build_q(c):
        @pl.loop(0, rows_c // 8)
        def _(t):
            for u in range(8):
                local = t * 8 + u
                row = pl.ds(c * rows_c + local, 1)
                ids = ids_v[row, :] - base
                qv = q_v[row, :]
                q_a = qv.astype(BF16).astype(F32)
                rest = qv - q_a
                q_b = rest.astype(BF16).astype(F32)
                q_c = rest - q_b
                hot_hi = lax.shift_right_arithmetic(ids, 7) == iota_hi
                hot_lo = jnp.where((ids & 127) == iota_lo, 1.0, 0.0).astype(BF16)
                parts = [jnp.where(hot_hi, part, 0.0).astype(BF16) for part in (q_a, q_b, q_c)]
                res = lax.dot_general(jnp.concatenate(parts, axis=0), hot_lo, NT, preferred_element_type=F32)
                dense = res[0:groups] + res[groups:2 * groups] + res[2 * groups:3 * groups]
                qs_v[pl.ds(local, groups, stride=rows_c), :] = dense

    def make_dz(c):
        @pl.loop(0, rows_c // 16)
        def _(i):
            off = al(i * 16, 16)
            rows = pl.ds(al(c * rows_c + off, 16), 16)
            lz = lz_v[rows, :]
            sn = sn_v[rows, :]
            acc = jnp.zeros((16, 128), F32)
            for k in range(groups):
                zz = z_v[rows, 128 * k:128 * (k + 1)]
                qq = qs_v[pl.ds(al(k * rows_c + off, 16), 16), :]
                acc = acc + qq * zz
                d = (jnp.exp(zz - lz) * sn - qq) * inv_tokens
                dz_v[rows, 128 * k:128 * (k + 1)] = d.astype(BF16)
            qz_v[...] = qz_v[...] + acc

    def make_dx(c):
        rows = slice(c * rows_c, (c + 1) * rows_c)

        @pl.loop(0, dim // 256)
        def _(j):
            cols = pl.ds(al(j * 256, 256), 256)
            dx_v[rows, cols] = jnp.dot(dz_v[rows, :], e_v[:, cols], preferred_element_type=F32)

    q8 = half // 8
    q4 = half // 4
    q2 = half // 2

    def rcopy(src, dst, c, slot, dev):
        return pltpu.make_async_remote_copy(
            src_ref=src, dst_ref=dst, send_sem=ss.at[c, slot], recv_sem=rs.at[c, slot],
            device_id=(dp, dev), device_id_type=MESH)

    def mine(c):
        return c * rows_c + half * core

    sent = []

    def go(*copies):
        for copy in copies:
            copy.start()
            sent.append(copy)

    def s0(c):
        return rcopy(dx_v.at[pl.ds(al(c * rows_c + half * (1 - core), half), half)], r0_v.at[c], c, 0, sib)

    def s1(c):
        a = rcopy(dx_v.at[pl.ds(al(mine(c) + q4 * (1 - xc), q4), q4)], r1_v.at[c, 0], c, 1, xn)
        b = rcopy(dx_v.at[pl.ds(al(mine(c) + q2 + q4 * (1 - yc), q4), q4)], r1_v.at[c, 1], c, 2, yn)
        return a, b

    def s2(c):
        a = rcopy(dx_v.at[pl.ds(al(mine(c) + q4 * xc + q8 * (1 - yc), q8), q8)], r2_v.at[c, 0], c, 3, yn)
        b = rcopy(dx_v.at[pl.ds(al(mine(c) + q2 + q4 * yc + q8 * (1 - xc), q8), q8)], r2_v.at[c, 1], c, 4, xn)
        return a, b

    def s3(c):
        rows_a = pl.ds(al(mine(c) + q4 * xc + q8 * yc, q8), q8)
        rows_b = pl.ds(al(mine(c) + q2 + q4 * yc + q8 * xc, q8), q8)
        return (rcopy(g_v.at[rows_a], g_v.at[rows_a], c, 5, yn), rcopy(g_v.at[rows_b], g_v.at[rows_b], c, 6, xn))

    def s4(c):
        rows_a = pl.ds(al(mine(c) + q4 * xc, q4), q4)
        rows_b = pl.ds(al(mine(c) + q2 + q4 * yc, q4), q4)
        return (rcopy(g_v.at[rows_a], g_v.at[rows_a], c, 7, xn), rcopy(g_v.at[rows_b], g_v.at[rows_b], c, 8, yn))

    def s5(c):
        rows = pl.ds(al(mine(c), half), half)
        return rcopy(g_v.at[rows], g_v.at[rows], c, 9, sib)

    def f0(c):
        go(s0(c))

    def f1(c):
        s0(c).wait_recv()

        @pl.loop(0, half // 8)
        def _(i):
            rows = pl.ds(al(mine(c) + 8 * i, 8), 8)
            dx_v[rows, :] = dx_v[rows, :] + r0_v[c, pl.ds(al(8 * i, 8), 8), :]
        go(*s1(c))

    def f2(c):
        a, b = s1(c)
        a.wait_recv()
        b.wait_recv()
        for k, start in ((0, mine(c) + q4 * xc), (1, mine(c) + q2 + q4 * yc)):
            rows = pl.ds(al(start, q4), q4)
            dx_v[rows, :] = dx_v[rows, :] + r1_v[c, k]
        go(*s2(c))

    def norm_back(c, k, block, side):
        rows16 = pl.ds(al(block, 16), 16)
        rows = pl.ds(al(block + q8 * side, q8), q8)
        hb = h_v[rows16, :].astype(F32)
        hf = jnp.where(side == 0, hb[0:8, :], hb[8:16, :])
        grad = dx_v[rows, :] + r2_v[c, k]
        inv = lax.rsqrt(jnp.mean(hf * hf, axis=1, keepdims=True) + 1e-6)
        scaled = grad * gain
        mean = jnp.sum(scaled * hf, axis=1, keepdims=True) * (1.0 / dim)
        g_v[rows, :] = scaled * inv - hf * (inv * inv * inv * mean)
        dwacc_v[...] = dwacc_v[...] + grad * hf * inv

    def f3(c):
        a, b = s2(c)
        a.wait_recv()
        b.wait_recv()
        norm_back(c, 0, mine(c) + q4 * xc, yc)
        norm_back(c, 1, mine(c) + q2 + q4 * yc, xc)
        go(*s3(c))

    def f4(c):
        a, b = s3(c)
        a.wait_recv()
        b.wait_recv()
        go(*s4(c))

    def f5(c):
        a, b = s4(c)
        a.wait_recv()
        b.wait_recv()
        go(s5(c))

    def rows_of(c):
        return slice(c * rows_c, (c + 1) * rows_c)

    def dh_copy(c):
        return pltpu.make_async_copy(dh_v.at[rows_of(c)], dh_hbm.at[rows_of(c)], out_sem.at[1 + c])

    def dz_copy(c):
        return pltpu.make_async_copy(dz_v.at[rows_of(c)], dz_hbm.at[rows_of(c)], out_sem.at[1 + CHUNKS + c])

    def f6(c):
        s5(c).wait_recv()

        @pl.loop(0, rows_c // 16)
        def _(i):
            rows = pl.ds(al(c * rows_c + 16 * i, 16), 16)
            dh_v[rows, :] = g_v[rows, :].astype(BF16)
        dh_copy(c).start()

    dwacc_v[...] = jnp.zeros(dwacc_v.shape, F32)
    qz_v[...] = jnp.zeros(qz_v.shape, F32)
    build_q(0)

    for copy in st_copies:
        copy.wait_recv()
    peak = st_recv[0][:, 0:tokens]
    for d in range(1, n_dev):
        peak = jnp.maximum(peak, st_recv[d][:, 0:tokens])
    total = jnp.zeros((1, tokens), F32)
    for d in range(n_dev):
        total = total + st_recv[d][:, tokens:2 * tokens] * jnp.exp(st_recv[d][:, 0:tokens] - peak)
    log_z = peak + jnp.log(total)
    for b in range(tokens // 128):
        lz_v[128 * b:128 * (b + 1), :] = jnp.broadcast_to(log_z[:, 128 * b:128 * (b + 1)], (128, 128)).T

    def chunk(c):
        make_dz(c)
        dz_copy(c).start()
        make_dx(c)

    chunk(0)
    f0(0)
    build_q(1)
    f1(0)
    chunk(1)
    f0(1)
    f2(0)
    build_q(2)
    f1(1)
    f3(0)
    chunk(2)
    f0(2)
    f2(1)
    f4(0)
    build_q(3)
    f1(2)
    f3(1)
    f5(0)
    chunk(3)
    f0(3)
    f2(2)
    f4(1)
    f6(0)
    f1(3)
    f3(2)
    f5(1)
    f2(3)
    f4(2)
    f6(1)
    f3(3)
    fin_send[:, 0:dim] = jnp.sum(dwacc_v[...], axis=0, keepdims=True)
    fin_send[:, dim:dim + 128] = jnp.sum(qz_v[...], axis=0, keepdims=True)
    fin_recv[me] = fin_send[...]
    fin_copies = gather_copies(fin_send, fin_recv, fin_ss, fin_rs)
    for copy in fin_copies:
        copy.start()
    f5(2)
    f4(3)
    f6(2)
    f5(3)

    for copy in fin_copies:
        copy.wait_recv()
    fin = fin_recv[0]
    for d in range(1, n_dev):
        fin = fin + fin_recv[d]
    dw_ref[...] = fin[:, 0:dim].reshape(dim)
    weighted = jnp.sum(lz_v[...] * sn_v[...], axis=0, keepdims=True)
    loss_ref[...] = (weighted - jnp.sum(fin[:, dim:dim + 128])) * inv_tokens
    f6(3)

    for copy in st_copies + sent + fin_copies:
        copy.wait_send()
    x_copy.wait()
    for c in range(CHUNKS):
        dz_copy(c).wait()
        dh_copy(c).wait()


def table_kernel(dz_hbm, x_hbm, out_hbm, dz_v, x_v, o_v, x_sem, dz_sem, out_sem):
    n_blk = out_hbm.shape[0] // VT

    def dz_copy(i):
        cols = pl.ds(pl.multiple_of(i * VT, VT), VT)
        return pltpu.make_async_copy(dz_hbm.at[:, cols], dz_v.at[:, cols], dz_sem.at[i])

    def out_copy(i):
        slot = lax.rem(i, SLOTS)
        return pltpu.make_async_copy(o_v.at[slot], out_hbm.at[pl.ds(pl.multiple_of(i * VT, VT), VT)], out_sem.at[slot])

    x_copy = pltpu.make_async_copy(x_hbm, x_v, x_sem)
    x_copy.start()

    @pl.loop(0, n_blk)
    def _(i):
        dz_copy(i).start()

    x_copy.wait()

    @pl.loop(0, n_blk)
    def _(i):
        dz_copy(i).wait()

        @pl.when(i >= SLOTS)
        def _():
            out_copy(i - SLOTS).wait()

        o_v[lax.rem(i, SLOTS)] = lax.dot_general(
            dz_v[:, pl.ds(pl.multiple_of(i * VT, VT), VT)], x_v[...], TN, preferred_element_type=F32)
        out_copy(i).start()

    for i in range(n_blk - SLOTS, n_blk):
        out_copy(i).wait()


def solution(mesh):
    n_dev = mesh.shape['tp']

    def local_step(hidden, norm_gain, emb_block, teacher_ids, teacher_q):
        tokens, dim = hidden.shape
        vocab = emb_block.shape[0]
        rows_c = tokens // CHUNKS
        half = rows_c // 2
        kt = teacher_ids.shape[1]
        any_spec = pl.BlockSpec(memory_space=pl.ANY)
        vmem_spec = pl.BlockSpec(memory_space=pltpu.VMEM)
        vm = pltpu.VMEM
        dma = pltpu.SemaphoreType.DMA
        dh, dw, loss, dz, x_in = pl.pallas_call(
            lambda *refs: fused_kernel(n_dev, *refs),
            out_shape=(
                jax.ShapeDtypeStruct((tokens, dim), BF16),
                jax.ShapeDtypeStruct((dim,), F32),
                jax.ShapeDtypeStruct((1, 128), F32),
                jax.ShapeDtypeStruct((tokens, vocab), BF16),
                jax.ShapeDtypeStruct((tokens, dim), BF16),
            ),
            in_specs=[any_spec, vmem_spec, any_spec, any_spec, any_spec],
            out_specs=(any_spec, vmem_spec, vmem_spec, any_spec, any_spec),
            scratch_shapes=[
                vm((tokens, dim), BF16),
                vm((tokens, dim), BF16),
                vm((vocab, dim), BF16),
                vm((tokens, kt), jnp.int32),
                vm((tokens, kt), F32),
                vm((tokens, vocab), F32),
                vm((tokens, 128), F32),
                vm((tokens, 128), F32),
                vm((tokens, 128), F32),
                vm((tokens, 128), F32),
                vm((vocab // 128 * rows_c, 128), F32),
                vm((tokens, vocab), BF16),
                vm((tokens, dim), F32),
                vm((tokens, dim), BF16),
                vm((tokens, dim), F32),
                vm((CHUNKS, half, dim), F32),
                vm((CHUNKS, 2, half // 4, dim), F32),
                vm((CHUNKS, 2, half // 8, dim), F32),
                vm((1, 2 * tokens), F32),
                vm((n_dev, 1, 2 * tokens), F32),
                vm((1, dim + 128), F32),
                vm((n_dev, 1, dim + 128), F32),
                vm((8, dim), F32),
                vm((16, 128), F32),
                dma((vocab // VT,)),
                dma((3,)),
                dma((1 + 2 * CHUNKS,)),
                dma((n_dev - 1,)),
                dma((n_dev - 1,)),
                dma((n_dev - 1,)),
                dma((n_dev - 1,)),
                dma((CHUNKS, 10)),
                dma((CHUNKS, 10)),
            ],
            compiler_params=pltpu.CompilerParams(
                collective_id=0, has_side_effects=True, vmem_limit_bytes=67_043_328),
            name='fused_head',
        )(hidden, norm_gain, emb_block, teacher_ids, teacher_q)
        grad_block = pl.pallas_call(
            table_kernel,
            in_specs=[any_spec, any_spec],
            out_specs=any_spec,
            out_shape=jax.ShapeDtypeStruct((vocab, dim), F32),
            scratch_shapes=[
                vm((tokens, vocab), BF16),
                vm((tokens, dim), BF16),
                vm((SLOTS, VT, dim), F32),
                dma,
                dma((vocab // VT,)),
                dma((SLOTS,)),
            ],
            compiler_params=pltpu.CompilerParams(vmem_limit_bytes=67_043_328),
            name='table_grad',
        )(dz, x_in)
        return (loss[0, 0:1], dh, dw, grad_block)

    return jax.shard_map(local_step, mesh=mesh, in_specs=(P('dp', None), P(None), P('tp', None), P('dp', None), P('dp', None)), out_specs=(P('dp'), P('dp', None), P('dp'), P(('dp', 'tp'), None)), check_vma=False)
```

```python
import jax
import jax.numpy as jnp
from jax import lax
from jax.experimental import pallas as pl
from jax.experimental.pallas import tpu as pltpu
from jax.sharding import PartitionSpec as P

MESH = pl.DeviceIdType.MESH
F32 = jnp.float32
BF16 = jnp.bfloat16
NT = (((1,), (1,)), ((), ()))
TN = (((0,), (0,)), ((), ()))
CHUNKS = 4
VT = 256
SLOTS = 3
TT = 512
TOK = 32


def fused_kernel(n_dev, h_hbm, w_ref, e_hbm, ids_hbm, q_hbm,
                 dh_hbm, dw_ref, loss_ref, dz_hbm, x_hbm,
                 h_v, x_v, e_v, ids_v, q_v, z_v, mx_v, sm_v, lz_v, sn_v, qs_v, dz_v, dx_v, dh_v, g_v,
                 r0_v, r1_v, r2_v, st_send, st_recv, fin_send, fin_recv, dwacc_v, qz_v,
                 e_sem, in_sem, out_sem, st_ss, st_rs, fin_ss, fin_rs, ss, rs):
    tokens, dim = h_v.shape
    vocab = e_v.shape[0]
    rows_c = tokens // CHUNKS
    groups = vocab // 128
    half = rows_c // 2
    n_blk = vocab // VT
    me = lax.axis_index('tp')
    dp = lax.axis_index('dp')
    core = me % 2
    xc = (me // 2) % 2
    yc = me // 4
    sib = me + 1 - 2 * core
    xn = me + 2 - 4 * xc
    yn = me + 4 - 8 * yc
    base = me * vocab
    inv_tokens = 1.0 / tokens

    def al(value, mult):
        return pl.multiple_of(value, mult)

    h_copy = pltpu.make_async_copy(h_hbm, h_v, in_sem.at[0])
    ids_copy = pltpu.make_async_copy(ids_hbm, ids_v, in_sem.at[1])
    q_copy = pltpu.make_async_copy(q_hbm, q_v, in_sem.at[2])
    q_copy.start()
    h_copy.start()

    def e_copy(i):
        rows = pl.ds(al(i * VT, VT), VT)
        return pltpu.make_async_copy(e_hbm.at[rows], e_v.at[rows], e_sem.at[i])

    @pl.loop(0, n_blk)
    def _(i):
        e_copy(i).start()

    ids_copy.start()

    barrier = pltpu.get_barrier_semaphore()
    for i in range(1, n_dev):
        pl.semaphore_signal(barrier, inc=1, device_id=(dp, (me + i) % n_dev), device_id_type=MESH)

    q_copy.wait()

    @pl.loop(0, tokens // 64)
    def _(i):
        rows = pl.ds(al(i * 64, 64), 64)
        sn_v[rows, :] = jnp.broadcast_to(jnp.sum(q_v[rows, :], axis=1, keepdims=True), (64, 128))

    h_copy.wait()
    gain = w_ref[...].reshape(1, dim) + 1.0

    @pl.loop(0, tokens // 64)
    def _(i):
        rows = pl.ds(al(i * 64, 64), 64)
        acc = jnp.zeros((64, 128), F32)
        for k in range(dim // 128):
            hf = h_v[rows, 128 * k:128 * (k + 1)].astype(F32)
            acc = acc + hf * hf
        inv = lax.rsqrt(jnp.sum(acc, axis=1, keepdims=True) * (1.0 / dim) + 1e-6)
        inv = jnp.broadcast_to(inv, (64, 128))
        for k in range(dim // 128):
            hf = h_v[rows, 128 * k:128 * (k + 1)].astype(F32)
            x_v[rows, 128 * k:128 * (k + 1)] = (hf * inv * gain[:, 128 * k:128 * (k + 1)]).astype(BF16)

    x_copy = pltpu.make_async_copy(x_v, x_hbm, out_sem.at[0])
    x_copy.start()

    mx_v[...] = jnp.full(mx_v.shape, -jnp.inf, F32)
    sm_v[...] = jnp.zeros(sm_v.shape, F32)

    @pl.loop(0, n_blk)
    def _(i):
        e_copy(i).wait()
        zb = lax.dot_general(x_v[...], e_v[pl.ds(al(i * VT, VT), VT), :], NT, preferred_element_type=F32)
        z_v[:, pl.ds(al(i * VT, VT), VT)] = zb
        old = mx_v[...]
        new = old
        for k in range(VT // 128):
            new = jnp.maximum(new, zb[:, 128 * k:128 * (k + 1)])
        total = sm_v[...] * jnp.exp(old - new)
        for k in range(VT // 128):
            total = total + jnp.exp(zb[:, 128 * k:128 * (k + 1)] - new)
        mx_v[...] = new
        sm_v[...] = total

    for b in range(tokens // 128):
        span = slice(128 * b, 128 * (b + 1))
        peaks = mx_v[span, :].T
        peak = jnp.max(peaks, axis=0, keepdims=True)
        st_send[:, 128 * b:128 * (b + 1)] = peak
        st_send[:, tokens + 128 * b:tokens + 128 * (b + 1)] = jnp.sum(
            sm_v[span, :].T * jnp.exp(peaks - peak), axis=0, keepdims=True)
    st_recv[me] = st_send[...]

    pl.semaphore_wait(barrier, n_dev - 1)

    def gather_copies(src, dst, s_sem, r_sem):
        out = []
        for i in range(1, n_dev):
            out.append(pltpu.make_async_remote_copy(
                src_ref=src, dst_ref=dst.at[me], send_sem=s_sem.at[i - 1], recv_sem=r_sem.at[i - 1],
                device_id=(dp, (me + i) % n_dev), device_id_type=MESH))
        return out

    st_copies = gather_copies(st_send, st_recv, st_ss, st_rs)
    for copy in st_copies:
        copy.start()

    ids_copy.wait()

    iota_hi = lax.broadcasted_iota(jnp.int32, (groups, 256), 0)
    iota_lo = lax.broadcasted_iota(jnp.int32, (128, 256), 0)

    def build_q(c):
        @pl.loop(0, rows_c // TOK)
        def _(t):
            for u in range(TOK):
                local = t * TOK + u
                row = pl.ds(c * rows_c + local, 1)
                ids = ids_v[row, :] - base
                qv = q_v[row, :]
                q_a = qv.astype(BF16).astype(F32)
                rest = qv - q_a
                q_b = rest.astype(BF16).astype(F32)
                q_c = rest - q_b
                hot_hi = lax.shift_right_arithmetic(ids, 7) == iota_hi
                hot_lo = jnp.where((ids & 127) == iota_lo, 1.0, 0.0).astype(BF16)
                parts = [jnp.where(hot_hi, part, 0.0).astype(BF16) for part in (q_a, q_b, q_c)]
                res = lax.dot_general(jnp.concatenate(parts, axis=0), hot_lo, NT, preferred_element_type=F32)
                dense = res[0:groups] + res[groups:2 * groups] + res[2 * groups:3 * groups]
                qs_v[pl.ds(local, groups, stride=rows_c), :] = dense

    def make_dz(c):
        @pl.loop(0, rows_c // 16)
        def _(i):
            off = al(i * 16, 16)
            rows = pl.ds(al(c * rows_c + off, 16), 16)
            lz = lz_v[rows, :]
            sn = sn_v[rows, :]
            acc = jnp.zeros((16, 128), F32)
            for k in range(groups):
                zz = z_v[rows, 128 * k:128 * (k + 1)]
                qq = qs_v[pl.ds(al(k * rows_c + off, 16), 16), :]
                acc = acc + qq * zz
                d = (jnp.exp(zz - lz) * sn - qq) * inv_tokens
                dz_v[rows, 128 * k:128 * (k + 1)] = d.astype(BF16)
            qz_v[...] = qz_v[...] + acc

    def make_dx(c):
        rows = slice(c * rows_c, (c + 1) * rows_c)

        @pl.loop(0, dim // 256)
        def _(j):
            cols = pl.ds(al(j * 256, 256), 256)
            dx_v[rows, cols] = jnp.dot(dz_v[rows, :], e_v[:, cols], preferred_element_type=F32)

    q8 = half // 8
    q4 = half // 4
    q2 = half // 2

    def rcopy(src, dst, c, slot, dev):
        return pltpu.make_async_remote_copy(
            src_ref=src, dst_ref=dst, send_sem=ss.at[c, slot], recv_sem=rs.at[c, slot],
            device_id=(dp, dev), device_id_type=MESH)

    def mine(c):
        return c * rows_c + half * core

    sent = []

    def go(*copies):
        for copy in copies:
            copy.start()
            sent.append(copy)

    def s0(c):
        return rcopy(dx_v.at[pl.ds(al(c * rows_c + half * (1 - core), half), half)], r0_v.at[c], c, 0, sib)

    def s1(c):
        a = rcopy(dx_v.at[pl.ds(al(mine(c) + q4 * (1 - xc), q4), q4)], r1_v.at[c, 0], c, 1, xn)
        b = rcopy(dx_v.at[pl.ds(al(mine(c) + q2 + q4 * (1 - yc), q4), q4)], r1_v.at[c, 1], c, 2, yn)
        return a, b

    def s2(c):
        a = rcopy(dx_v.at[pl.ds(al(mine(c) + q4 * xc + q8 * (1 - yc), q8), q8)], r2_v.at[c, 0], c, 3, yn)
        b = rcopy(dx_v.at[pl.ds(al(mine(c) + q2 + q4 * yc + q8 * (1 - xc), q8), q8)], r2_v.at[c, 1], c, 4, xn)
        return a, b

    def s3(c):
        rows_a = pl.ds(al(mine(c) + q4 * xc + q8 * yc, q8), q8)
        rows_b = pl.ds(al(mine(c) + q2 + q4 * yc + q8 * xc, q8), q8)
        return (rcopy(g_v.at[rows_a], g_v.at[rows_a], c, 5, yn), rcopy(g_v.at[rows_b], g_v.at[rows_b], c, 6, xn))

    def s4(c):
        rows_a = pl.ds(al(mine(c) + q4 * xc, q4), q4)
        rows_b = pl.ds(al(mine(c) + q2 + q4 * yc, q4), q4)
        return (rcopy(g_v.at[rows_a], g_v.at[rows_a], c, 7, xn), rcopy(g_v.at[rows_b], g_v.at[rows_b], c, 8, yn))

    def s5(c):
        rows = pl.ds(al(mine(c), half), half)
        return rcopy(g_v.at[rows], g_v.at[rows], c, 9, sib)

    def f0(c):
        go(s0(c))

    def f1(c):
        s0(c).wait_recv()

        @pl.loop(0, half // 8)
        def _(i):
            rows = pl.ds(al(mine(c) + 8 * i, 8), 8)
            dx_v[rows, :] = dx_v[rows, :] + r0_v[c, pl.ds(al(8 * i, 8), 8), :]
        go(*s1(c))

    def f2(c):
        a, b = s1(c)
        a.wait_recv()
        b.wait_recv()
        for k, start in ((0, mine(c) + q4 * xc), (1, mine(c) + q2 + q4 * yc)):
            rows = pl.ds(al(start, q4), q4)
            dx_v[rows, :] = dx_v[rows, :] + r1_v[c, k]
        go(*s2(c))

    def norm_back(c, k, block, side):
        rows16 = pl.ds(al(block, 16), 16)
        rows = pl.ds(al(block + q8 * side, q8), q8)
        hb = h_v[rows16, :].astype(F32)
        hf = jnp.where(side == 0, hb[0:8, :], hb[8:16, :])
        grad = dx_v[rows, :] + r2_v[c, k]
        inv = lax.rsqrt(jnp.mean(hf * hf, axis=1, keepdims=True) + 1e-6)
        scaled = grad * gain
        mean = jnp.sum(scaled * hf, axis=1, keepdims=True) * (1.0 / dim)
        g_v[rows, :] = scaled * inv - hf * (inv * inv * inv * mean)
        dwacc_v[...] = dwacc_v[...] + grad * hf * inv

    def f3(c):
        a, b = s2(c)
        a.wait_recv()
        b.wait_recv()
        norm_back(c, 0, mine(c) + q4 * xc, yc)
        norm_back(c, 1, mine(c) + q2 + q4 * yc, xc)
        go(*s3(c))

    def f4(c):
        a, b = s3(c)
        a.wait_recv()
        b.wait_recv()
        go(*s4(c))

    def f5(c):
        a, b = s4(c)
        a.wait_recv()
        b.wait_recv()
        go(s5(c))

    def rows_of(c):
        return slice(c * rows_c, (c + 1) * rows_c)

    def dh_copy(c):
        return pltpu.make_async_copy(dh_v.at[rows_of(c)], dh_hbm.at[rows_of(c)], out_sem.at[1 + c])

    def dz_copy(c):
        return pltpu.make_async_copy(dz_v.at[rows_of(c)], dz_hbm.at[rows_of(c)], out_sem.at[1 + CHUNKS + c])

    def f6(c):
        s5(c).wait_recv()

        @pl.loop(0, rows_c // 16)
        def _(i):
            rows = pl.ds(al(c * rows_c + 16 * i, 16), 16)
            dh_v[rows, :] = g_v[rows, :].astype(BF16)
        dh_copy(c).start()

    dwacc_v[...] = jnp.zeros(dwacc_v.shape, F32)
    qz_v[...] = jnp.zeros(qz_v.shape, F32)
    build_q(0)

    for copy in st_copies:
        copy.wait_recv()
    peak = st_recv[0][:, 0:tokens]
    for d in range(1, n_dev):
        peak = jnp.maximum(peak, st_recv[d][:, 0:tokens])
    total = jnp.zeros((1, tokens), F32)
    for d in range(n_dev):
        total = total + st_recv[d][:, tokens:2 * tokens] * jnp.exp(st_recv[d][:, 0:tokens] - peak)
    log_z = peak + jnp.log(total)
    for b in range(tokens // 128):
        lz_v[128 * b:128 * (b + 1), :] = jnp.broadcast_to(log_z[:, 128 * b:128 * (b + 1)], (128, 128)).T

    def chunk(c):
        make_dz(c)
        dz_copy(c).start()
        make_dx(c)

    chunk(0)
    f0(0)
    build_q(1)
    f1(0)
    chunk(1)
    f0(1)
    f2(0)
    build_q(2)
    f1(1)
    f3(0)
    chunk(2)
    f0(2)
    f2(1)
    f4(0)
    build_q(3)
    f1(2)
    f3(1)
    f5(0)
    chunk(3)
    f0(3)
    f2(2)
    f4(1)
    f6(0)
    f1(3)
    f3(2)
    f5(1)
    f2(3)
    f4(2)
    f6(1)
    f3(3)
    fin_send[:, 0:dim] = jnp.sum(dwacc_v[...], axis=0, keepdims=True)
    fin_send[:, dim:dim + 128] = jnp.sum(qz_v[...], axis=0, keepdims=True)
    fin_recv[me] = fin_send[...]
    fin_copies = gather_copies(fin_send, fin_recv, fin_ss, fin_rs)
    for copy in fin_copies:
        copy.start()
    f5(2)
    f4(3)
    f6(2)
    f5(3)

    for copy in fin_copies:
        copy.wait_recv()
    fin = fin_recv[0]
    for d in range(1, n_dev):
        fin = fin + fin_recv[d]
    dw_ref[...] = fin[:, 0:dim].reshape(dim)
    weighted = jnp.sum(lz_v[...] * sn_v[...], axis=0, keepdims=True)
    loss_ref[...] = (weighted - jnp.sum(fin[:, dim:dim + 128])) * inv_tokens
    f6(3)

    for copy in st_copies + sent + fin_copies:
        copy.wait_send()
    x_copy.wait()
    for c in range(CHUNKS):
        dz_copy(c).wait()
        dh_copy(c).wait()


def table_kernel(dz_hbm, x_hbm, dh_hbm, dw_ref, loss_ref, out_hbm, dh_out, dw_out, loss_out,
                 dz_v, x_v, o_v, dh_v, x_sem, dz_sem, out_sem, dh_sem):
    n_blk = out_hbm.shape[0] // TT
    half = out_hbm.shape[1] // 2
    cuts = (slice(0, half), slice(half, 2 * half))

    def dz_copy(i):
        cols = pl.ds(pl.multiple_of(i * TT, TT), TT)
        return pltpu.make_async_copy(dz_hbm.at[:, cols], dz_v.at[:, cols], dz_sem.at[i])

    def out_copy(i, k):
        slot = lax.rem(i, SLOTS)
        rows = pl.ds(pl.multiple_of(i * TT, TT), TT)
        return pltpu.make_async_copy(o_v.at[slot, :, cuts[k]], out_hbm.at[rows, cuts[k]], out_sem.at[slot, k])

    x_copy = pltpu.make_async_copy(x_hbm, x_v, x_sem)
    x_copy.start()

    @pl.loop(0, n_blk)
    def _(i):
        dz_copy(i).start()

    dh_in = pltpu.make_async_copy(dh_hbm, dh_v, dh_sem.at[0])
    dh_put = pltpu.make_async_copy(dh_v, dh_out, dh_sem.at[1])
    dh_in.start()
    dw_out[...] = dw_ref[...]
    loss_out[...] = loss_ref[...]
    x_copy.wait()

    @pl.loop(0, n_blk)
    def _(i):
        dz_copy(i).wait()

        @pl.when(i >= SLOTS)
        def _():
            out_copy(i - SLOTS, 0).wait()
            out_copy(i - SLOTS, 1).wait()

        cols = pl.ds(pl.multiple_of(i * TT, TT), TT)
        for k in range(2):
            o_v[lax.rem(i, SLOTS), :, cuts[k]] = lax.dot_general(
                dz_v[:, cols], x_v[:, cuts[k]], TN, preferred_element_type=F32)
            out_copy(i, k).start()

        @pl.when(i == 1)
        def _():
            dh_in.wait()
            dh_put.start()

    for i in range(n_blk - SLOTS, n_blk):
        out_copy(i, 0).wait()
        out_copy(i, 1).wait()
    dh_put.wait()


def solution(mesh):
    n_dev = mesh.shape['tp']

    def local_step(hidden, norm_gain, emb_block, teacher_ids, teacher_q):
        tokens, dim = hidden.shape
        vocab = emb_block.shape[0]
        rows_c = tokens // CHUNKS
        half = rows_c // 2
        kt = teacher_ids.shape[1]
        any_spec = pl.BlockSpec(memory_space=pl.ANY)
        vmem_spec = pl.BlockSpec(memory_space=pltpu.VMEM)
        vm = pltpu.VMEM
        dma = pltpu.SemaphoreType.DMA
        dh, dw, loss, dz, x_in = pl.pallas_call(
            lambda *refs: fused_kernel(n_dev, *refs),
            out_shape=(
                jax.ShapeDtypeStruct((tokens, dim), BF16),
                jax.ShapeDtypeStruct((dim,), F32),
                jax.ShapeDtypeStruct((1, 128), F32),
                jax.ShapeDtypeStruct((tokens, vocab), BF16),
                jax.ShapeDtypeStruct((tokens, dim), BF16),
            ),
            in_specs=[any_spec, vmem_spec, any_spec, any_spec, any_spec],
            out_specs=(any_spec, vmem_spec, vmem_spec, any_spec, any_spec),
            scratch_shapes=[
                vm((tokens, dim), BF16),
                vm((tokens, dim), BF16),
                vm((vocab, dim), BF16),
                vm((tokens, kt), jnp.int32),
                vm((tokens, kt), F32),
                vm((tokens, vocab), F32),
                vm((tokens, 128), F32),
                vm((tokens, 128), F32),
                vm((tokens, 128), F32),
                vm((tokens, 128), F32),
                vm((vocab // 128 * rows_c, 128), F32),
                vm((tokens, vocab), BF16),
                vm((tokens, dim), F32),
                vm((tokens, dim), BF16),
                vm((tokens, dim), F32),
                vm((CHUNKS, half, dim), F32),
                vm((CHUNKS, 2, half // 4, dim), F32),
                vm((CHUNKS, 2, half // 8, dim), F32),
                vm((1, 2 * tokens), F32),
                vm((n_dev, 1, 2 * tokens), F32),
                vm((1, dim + 128), F32),
                vm((n_dev, 1, dim + 128), F32),
                vm((8, dim), F32),
                vm((16, 128), F32),
                dma((vocab // VT,)),
                dma((3,)),
                dma((1 + 2 * CHUNKS,)),
                dma((n_dev - 1,)),
                dma((n_dev - 1,)),
                dma((n_dev - 1,)),
                dma((n_dev - 1,)),
                dma((CHUNKS, 10)),
                dma((CHUNKS, 10)),
            ],
            compiler_params=pltpu.CompilerParams(
                collective_id=0, has_side_effects=True, vmem_limit_bytes=67_043_328),
            name='fused_head',
        )(hidden, norm_gain, emb_block, teacher_ids, teacher_q)
        grad_block, dh, dw, loss = pl.pallas_call(
            table_kernel,
            in_specs=[any_spec, any_spec, any_spec, vmem_spec, vmem_spec],
            out_specs=(any_spec, any_spec, vmem_spec, vmem_spec),
            out_shape=(
                jax.ShapeDtypeStruct((vocab, dim), F32),
                jax.ShapeDtypeStruct((tokens, dim), BF16),
                jax.ShapeDtypeStruct((dim,), F32),
                jax.ShapeDtypeStruct((1, 128), F32),
            ),
            scratch_shapes=[
                vm((tokens, vocab), BF16),
                vm((tokens, dim), BF16),
                vm((SLOTS, TT, dim), F32),
                vm((tokens, dim), BF16),
                dma,
                dma((vocab // TT,)),
                dma((SLOTS, 2)),
                dma((2,)),
            ],
            compiler_params=pltpu.CompilerParams(vmem_limit_bytes=67_043_328),
            name='table_grad',
        )(dz, x_in, dh, dw, loss)
        return (loss[0, 0:1], dh, dw, grad_block)

    return jax.shard_map(local_step, mesh=mesh, in_specs=(P('dp', None), P(None), P('tp', None), P('dp', None), P('dp', None)), out_specs=(P('dp'), P('dp', None), P('dp'), P(('dp', 'tp'), None)), check_vma=False)
```

```python
import jax
import jax.numpy as jnp
from jax import lax
from jax.experimental import pallas as pl
from jax.experimental.pallas import tpu as pltpu
from jax.sharding import PartitionSpec as P

MESH = pl.DeviceIdType.MESH
F32 = jnp.float32
BF16 = jnp.bfloat16
NT = (((1,), (1,)), ((), ()))
TN = (((0,), (0,)), ((), ()))
CHUNKS = 4
HALVES = 2
VT = 256
SLOTS = 3
TT = 512
TOK = 32


def fused_kernel(n_dev, h_hbm, w_ref, e_hbm, ids_hbm, q_hbm,
                 dh_hbm, dw_ref, loss_ref, dz_hbm, x_hbm,
                 h_v, x_v, e_v, ids_v, q_v, z_v, mx_v, sm_v, lz_v, sn_v, qs_v, dz_v, dx_v, dh_v, g_v,
                 r0_v, r1_v, r2_v, st_send, st_recv, fin_send, fin_recv, dwacc_v, qz_v,
                 e_sem, in_sem, out_sem, st_ss, st_rs, fin_ss, fin_rs, ss, rs):
    tokens, dim = h_v.shape
    vocab = e_v.shape[0]
    rows_c = tokens // CHUNKS
    groups = vocab // 128
    half = rows_c // 2
    n_blk = vocab // VT
    me = lax.axis_index('tp')
    dp = lax.axis_index('dp')
    core = me % 2
    xc = (me // 2) % 2
    yc = me // 4
    sib = me + 1 - 2 * core
    xn = me + 2 - 4 * xc
    yn = me + 4 - 8 * yc
    base = me * vocab
    inv_tokens = 1.0 / tokens

    def al(value, mult):
        return pl.multiple_of(value, mult)

    h_copy = pltpu.make_async_copy(h_hbm, h_v, in_sem.at[0])
    ids_copy = pltpu.make_async_copy(ids_hbm, ids_v, in_sem.at[1])
    q_copy = pltpu.make_async_copy(q_hbm, q_v, in_sem.at[2])
    q_copy.start()
    h_copy.start()

    def e_copy(i):
        rows = pl.ds(al(i * VT, VT), VT)
        return pltpu.make_async_copy(e_hbm.at[rows], e_v.at[rows], e_sem.at[i])

    @pl.loop(0, n_blk)
    def _(i):
        e_copy(i).start()

    ids_copy.start()

    barrier = pltpu.get_barrier_semaphore()
    for i in range(1, n_dev):
        pl.semaphore_signal(barrier, inc=1, device_id=(dp, (me + i) % n_dev), device_id_type=MESH)

    q_copy.wait()

    @pl.loop(0, tokens // 64)
    def _(i):
        rows = pl.ds(al(i * 64, 64), 64)
        sn_v[rows, :] = jnp.broadcast_to(jnp.sum(q_v[rows, :], axis=1, keepdims=True), (64, 128))

    h_copy.wait()
    gain = w_ref[...].reshape(1, dim) + 1.0

    part = tokens // HALVES

    def norm(h):
        @pl.loop(0, part // 64)
        def _(i):
            rows = pl.ds(al(h * part + i * 64, 64), 64)
            acc = jnp.zeros((64, 128), F32)
            for k in range(dim // 128):
                hf = h_v[rows, 128 * k:128 * (k + 1)].astype(F32)
                acc = acc + hf * hf
            inv = lax.rsqrt(jnp.sum(acc, axis=1, keepdims=True) * (1.0 / dim) + 1e-6)
            inv = jnp.broadcast_to(inv, (64, 128))
            for k in range(dim // 128):
                hf = h_v[rows, 128 * k:128 * (k + 1)].astype(F32)
                x_v[rows, 128 * k:128 * (k + 1)] = (hf * inv * gain[:, 128 * k:128 * (k + 1)]).astype(BF16)

    mx_v[...] = jnp.full(mx_v.shape, -jnp.inf, F32)
    sm_v[...] = jnp.zeros(sm_v.shape, F32)

    def logits(h, first, last):
        rows = slice(h * part, (h + 1) * part)

        @pl.loop(first, last)
        def _(i):
            if h == 0:
                e_copy(i).wait()
            zb = lax.dot_general(x_v[rows, :], e_v[pl.ds(al(i * VT, VT), VT), :], NT, preferred_element_type=F32)
            z_v[rows, pl.ds(al(i * VT, VT), VT)] = zb
            old = mx_v[rows, :]
            new = old
            for k in range(VT // 128):
                new = jnp.maximum(new, zb[:, 128 * k:128 * (k + 1)])
            total = sm_v[rows, :] * jnp.exp(old - new)
            for k in range(VT // 128):
                total = total + jnp.exp(zb[:, 128 * k:128 * (k + 1)] - new)
            mx_v[rows, :] = new
            sm_v[rows, :] = total

    def gather_copies(src, dst, s_sem, r_sem):
        out = []
        for i in range(1, n_dev):
            out.append(pltpu.make_async_remote_copy(
                src_ref=src, dst_ref=dst.at[me], send_sem=s_sem.at[i - 1], recv_sem=r_sem.at[i - 1],
                device_id=(dp, (me + i) % n_dev), device_id_type=MESH))
        return out

    st_copies = [gather_copies(st_send.at[h], st_recv.at[h], st_ss.at[h], st_rs.at[h]) for h in range(HALVES)]

    def send_stats(h):
        for b in range(part // 128):
            span = slice(h * part + 128 * b, h * part + 128 * (b + 1))
            peaks = mx_v[span, :].T
            peak = jnp.max(peaks, axis=0, keepdims=True)
            st_send[h, :, 128 * b:128 * (b + 1)] = peak
            st_send[h, :, part + 128 * b:part + 128 * (b + 1)] = jnp.sum(
                sm_v[span, :].T * jnp.exp(peaks - peak), axis=0, keepdims=True)
        st_recv[h, me] = st_send[h]
        if h == 0:
            pl.semaphore_wait(barrier, n_dev - 1)
        for copy in st_copies[h]:
            copy.start()

    def take_stats(h):
        for copy in st_copies[h]:
            copy.wait_recv()
        peak = st_recv[h, 0][:, 0:part]
        for d in range(1, n_dev):
            peak = jnp.maximum(peak, st_recv[h, d][:, 0:part])
        total = jnp.zeros((1, part), F32)
        for d in range(n_dev):
            total = total + st_recv[h, d][:, part:2 * part] * jnp.exp(st_recv[h, d][:, 0:part] - peak)
        log_z = peak + jnp.log(total)
        for b in range(part // 128):
            lz_v[h * part + 128 * b:h * part + 128 * (b + 1), :] = jnp.broadcast_to(
                log_z[:, 128 * b:128 * (b + 1)], (128, 128)).T

    norm(0)
    logits(0, 0, n_blk)
    send_stats(0)
    norm(1)
    x_copy = pltpu.make_async_copy(x_v, x_hbm, out_sem.at[0])
    x_copy.start()
    ids_copy.wait()

    iota_hi = lax.broadcasted_iota(jnp.int32, (groups, 256), 0)
    iota_lo = lax.broadcasted_iota(jnp.int32, (128, 256), 0)

    def build_q(c, p):
        @pl.loop(p * rows_c // TOK // 2, (p + 1) * rows_c // TOK // 2)
        def _(t):
            for u in range(TOK):
                local = t * TOK + u
                row = pl.ds(c * rows_c + local, 1)
                ids = ids_v[row, :] - base
                qv = q_v[row, :]
                q_a = qv.astype(BF16).astype(F32)
                rest = qv - q_a
                q_b = rest.astype(BF16).astype(F32)
                q_c = rest - q_b
                hot_hi = lax.shift_right_arithmetic(ids, 7) == iota_hi
                hot_lo = jnp.where((ids & 127) == iota_lo, 1.0, 0.0).astype(BF16)
                parts = [jnp.where(hot_hi, part, 0.0).astype(BF16) for part in (q_a, q_b, q_c)]
                res = lax.dot_general(jnp.concatenate(parts, axis=0), hot_lo, NT, preferred_element_type=F32)
                dense = res[0:groups] + res[groups:2 * groups] + res[2 * groups:3 * groups]
                qs_v[pl.ds(local, groups, stride=rows_c), :] = dense

    def make_dz(c):
        @pl.loop(0, rows_c // 16)
        def _(i):
            off = al(i * 16, 16)
            rows = pl.ds(al(c * rows_c + off, 16), 16)
            lz = lz_v[rows, :]
            sn = sn_v[rows, :]
            acc = jnp.zeros((16, 128), F32)
            for k in range(groups):
                zz = z_v[rows, 128 * k:128 * (k + 1)]
                qq = qs_v[pl.ds(al(k * rows_c + off, 16), 16), :]
                acc = acc + qq * zz
                d = (jnp.exp(zz - lz) * sn - qq) * inv_tokens
                dz_v[rows, 128 * k:128 * (k + 1)] = d.astype(BF16)
            qz_v[...] = qz_v[...] + acc

    def make_dx(c, p):
        rows = slice(c * rows_c, (c + 1) * rows_c)

        @pl.loop(p * dim // 256 // 2, (p + 1) * dim // 256 // 2)
        def _(j):
            cols = pl.ds(al(j * 256, 256), 256)
            dx_v[rows, cols] = jnp.dot(dz_v[rows, :], e_v[:, cols], preferred_element_type=F32)

    q8 = half // 8
    q4 = half // 4
    q2 = half // 2

    wide = dim // 2
    cut = (slice(0, wide), slice(wide, 2 * wide))

    def rcopy(src, dst, c, p, slot, dev):
        return pltpu.make_async_remote_copy(
            src_ref=src, dst_ref=dst, send_sem=ss.at[c, p, slot], recv_sem=rs.at[c, p, slot],
            device_id=(dp, dev), device_id_type=MESH)

    def mine(c):
        return c * rows_c + half * core

    sent = []

    def go(*copies):
        for copy in copies:
            copy.start()
            sent.append(copy)

    def dx_at(start, size, p):
        return dx_v.at[pl.ds(al(start, size), size), cut[p]]

    def g_at(start, size, p):
        return g_v.at[pl.ds(al(start, size), size), cut[p]]

    def s0(c, p):
        return rcopy(dx_at(c * rows_c + half * (1 - core), half, p), r0_v.at[c, :, cut[p]], c, p, 0, sib)

    def s1(c, p):
        a = rcopy(dx_at(mine(c) + q4 * (1 - xc), q4, p), r1_v.at[c, 0, :, cut[p]], c, p, 1, xn)
        b = rcopy(dx_at(mine(c) + q2 + q4 * (1 - yc), q4, p), r1_v.at[c, 1, :, cut[p]], c, p, 2, yn)
        return a, b

    def s2(c, p):
        a = rcopy(dx_at(mine(c) + q4 * xc + q8 * (1 - yc), q8, p), r2_v.at[c, 0, :, cut[p]], c, p, 3, yn)
        b = rcopy(dx_at(mine(c) + q2 + q4 * yc + q8 * (1 - xc), q8, p), r2_v.at[c, 1, :, cut[p]], c, p, 4, xn)
        return a, b

    def s3(c, p):
        a = g_at(mine(c) + q4 * xc + q8 * yc, q8, p)
        b = g_at(mine(c) + q2 + q4 * yc + q8 * xc, q8, p)
        return rcopy(a, a, c, p, 5, yn), rcopy(b, b, c, p, 6, xn)

    def s4(c, p):
        a = g_at(mine(c) + q4 * xc, q4, p)
        b = g_at(mine(c) + q2 + q4 * yc, q4, p)
        return rcopy(a, a, c, p, 7, xn), rcopy(b, b, c, p, 8, yn)

    def s5(c, p):
        a = g_at(mine(c), half, p)
        return rcopy(a, a, c, p, 9, sib)

    def f0(c, p):
        go(s0(c, p))

    def f1(c, p):
        s0(c, p).wait_recv()

        @pl.loop(0, half // 8)
        def _(i):
            rows = pl.ds(al(mine(c) + 8 * i, 8), 8)
            dx_v[rows, cut[p]] = dx_v[rows, cut[p]] + r0_v[c, pl.ds(al(8 * i, 8), 8), cut[p]]
        go(*s1(c, p))

    def f2(c, p):
        for copy in s1(c, p):
            copy.wait_recv()
        for k, start in ((0, mine(c) + q4 * xc), (1, mine(c) + q2 + q4 * yc)):
            rows = pl.ds(al(start, q4), q4)
            dx_v[rows, cut[p]] = dx_v[rows, cut[p]] + r1_v[c, k, :, cut[p]]
        go(*s2(c, p))

    def norm_back(c, k, block, side):
        rows16 = pl.ds(al(block, 16), 16)
        rows = pl.ds(al(block + q8 * side, q8), q8)
        hb = h_v[rows16, :].astype(F32)
        hf = jnp.where(side == 0, hb[0:8, :], hb[8:16, :])
        grad = dx_v[rows, :] + r2_v[c, k]
        inv = lax.rsqrt(jnp.mean(hf * hf, axis=1, keepdims=True) + 1e-6)
        scaled = grad * gain
        mean = jnp.sum(scaled * hf, axis=1, keepdims=True) * (1.0 / dim)
        g_v[rows, :] = scaled * inv - hf * (inv * inv * inv * mean)
        dwacc_v[...] = dwacc_v[...] + grad * hf * inv

    def f3(c):
        for p in range(2):
            for copy in s2(c, p):
                copy.wait_recv()
        norm_back(c, 0, mine(c) + q4 * xc, yc)
        norm_back(c, 1, mine(c) + q2 + q4 * yc, xc)
        for p in range(2):
            go(*s3(c, p))

    def f4(c, p):
        for copy in s3(c, p):
            copy.wait_recv()
        go(*s4(c, p))

    def f5(c, p):
        for copy in s4(c, p):
            copy.wait_recv()
        go(s5(c, p))

    def rows_of(c):
        return slice(c * rows_c, (c + 1) * rows_c)

    def dh_copy(c):
        return pltpu.make_async_copy(dh_v.at[rows_of(c)], dh_hbm.at[rows_of(c)], out_sem.at[1 + c])

    def dz_copy(c):
        return pltpu.make_async_copy(dz_v.at[rows_of(c)], dz_hbm.at[rows_of(c)], out_sem.at[1 + CHUNKS + c])

    def f6(c):
        for p in range(2):
            s5(c, p).wait_recv()

        @pl.loop(0, rows_c // 16)
        def _(i):
            rows = pl.ds(al(c * rows_c + 16 * i, 16), 16)
            dh_v[rows, :] = g_v[rows, :].astype(BF16)
        dh_copy(c).start()

    dwacc_v[...] = jnp.zeros(dwacc_v.shape, F32)
    qz_v[...] = jnp.zeros(qz_v.shape, F32)

    def finish_dz(c):
        make_dz(c)
        dz_copy(c).start()

    quarter = n_blk // 4
    build_q(0, 0)
    build_q(0, 1)
    take_stats(0)
    finish_dz(0)
    make_dx(0, 0)
    f0(0, 0)
    make_dx(0, 1)
    f0(0, 1)
    f1(0, 0)
    build_q(1, 0)
    f1(0, 1)
    build_q(1, 1)
    f2(0, 0)
    finish_dz(1)
    f2(0, 1)
    make_dx(1, 0)
    f0(1, 0)
    make_dx(1, 1)
    f0(1, 1)
    f3(0)
    f1(1, 0)
    logits(1, 0, quarter)
    f1(1, 1)
    f4(0, 0)
    f4(0, 1)
    logits(1, quarter, 2 * quarter)
    f2(1, 0)
    logits(1, 2 * quarter, 3 * quarter)
    f2(1, 1)
    f5(0, 0)
    f5(0, 1)
    logits(1, 3 * quarter, n_blk)
    send_stats(1)
    f3(1)
    f6(0)
    build_q(2, 0)
    build_q(2, 1)
    f4(1, 0)
    f4(1, 1)
    take_stats(1)
    finish_dz(2)
    make_dx(2, 0)
    f0(2, 0)
    f5(1, 0)
    f5(1, 1)
    make_dx(2, 1)
    f0(2, 1)
    f1(2, 0)
    build_q(3, 0)
    f1(2, 1)
    build_q(3, 1)
    f2(2, 0)
    f6(1)
    finish_dz(3)
    f2(2, 1)
    make_dx(3, 0)
    f0(3, 0)
    make_dx(3, 1)
    f0(3, 1)
    f1(3, 0)
    f3(2)
    f1(3, 1)
    f2(3, 0)
    f4(2, 0)
    f4(2, 1)
    f2(3, 1)
    f5(2, 0)
    f5(2, 1)
    f3(3)
    fin_send[:, 0:dim] = jnp.sum(dwacc_v[...], axis=0, keepdims=True)
    fin_send[:, dim:dim + 128] = jnp.sum(qz_v[...], axis=0, keepdims=True)
    fin_recv[me] = fin_send[...]
    fin_copies = gather_copies(fin_send, fin_recv, fin_ss, fin_rs)
    for copy in fin_copies:
        copy.start()
    f4(3, 0)
    f4(3, 1)
    f6(2)
    f5(3, 0)
    f5(3, 1)

    for copy in fin_copies:
        copy.wait_recv()
    fin = fin_recv[0]
    for d in range(1, n_dev):
        fin = fin + fin_recv[d]
    dw_ref[...] = fin[:, 0:dim].reshape(dim)
    weighted = jnp.sum(lz_v[...] * sn_v[...], axis=0, keepdims=True)
    loss_ref[...] = (weighted - jnp.sum(fin[:, dim:dim + 128])) * inv_tokens
    f6(3)

    for copy in st_copies[0] + st_copies[1] + sent + fin_copies:
        copy.wait_send()
    x_copy.wait()
    for c in range(CHUNKS):
        dz_copy(c).wait()
        dh_copy(c).wait()


def table_kernel(dz_hbm, x_hbm, dh_hbm, dw_ref, loss_ref, out_hbm, dh_out, dw_out, loss_out,
                 dz_v, x_v, o_v, dh_v, x_sem, dz_sem, out_sem, dh_sem):
    n_blk = out_hbm.shape[0] // TT
    half = out_hbm.shape[1] // 2
    cuts = (slice(0, half), slice(half, 2 * half))

    def dz_copy(i):
        cols = pl.ds(pl.multiple_of(i * TT, TT), TT)
        return pltpu.make_async_copy(dz_hbm.at[:, cols], dz_v.at[:, cols], dz_sem.at[i])

    def out_copy(i, k):
        slot = lax.rem(i, SLOTS)
        rows = pl.ds(pl.multiple_of(i * TT, TT), TT)
        return pltpu.make_async_copy(o_v.at[slot, :, cuts[k]], out_hbm.at[rows, cuts[k]], out_sem.at[slot, k])

    x_copy = pltpu.make_async_copy(x_hbm, x_v, x_sem)
    x_copy.start()

    @pl.loop(0, n_blk)
    def _(i):
        dz_copy(i).start()

    dh_in = pltpu.make_async_copy(dh_hbm, dh_v, dh_sem.at[0])
    dh_put = pltpu.make_async_copy(dh_v, dh_out, dh_sem.at[1])
    dh_in.start()
    dw_out[...] = dw_ref[...]
    loss_out[...] = loss_ref[...]
    x_copy.wait()

    @pl.loop(0, n_blk)
    def _(i):
        dz_copy(i).wait()

        @pl.when(i >= SLOTS)
        def _():
            out_copy(i - SLOTS, 0).wait()
            out_copy(i - SLOTS, 1).wait()

        cols = pl.ds(pl.multiple_of(i * TT, TT), TT)
        for k in range(2):
            o_v[lax.rem(i, SLOTS), :, cuts[k]] = lax.dot_general(
                dz_v[:, cols], x_v[:, cuts[k]], TN, preferred_element_type=F32)
            out_copy(i, k).start()

        @pl.when(i == 1)
        def _():
            dh_in.wait()
            dh_put.start()

    for i in range(n_blk - SLOTS, n_blk):
        out_copy(i, 0).wait()
        out_copy(i, 1).wait()
    dh_put.wait()


def solution(mesh):
    n_dev = mesh.shape['tp']

    def local_step(hidden, norm_gain, emb_block, teacher_ids, teacher_q):
        tokens, dim = hidden.shape
        vocab = emb_block.shape[0]
        rows_c = tokens // CHUNKS
        half = rows_c // 2
        kt = teacher_ids.shape[1]
        any_spec = pl.BlockSpec(memory_space=pl.ANY)
        vmem_spec = pl.BlockSpec(memory_space=pltpu.VMEM)
        vm = pltpu.VMEM
        dma = pltpu.SemaphoreType.DMA
        dh, dw, loss, dz, x_in = pl.pallas_call(
            lambda *refs: fused_kernel(n_dev, *refs),
            out_shape=(
                jax.ShapeDtypeStruct((tokens, dim), BF16),
                jax.ShapeDtypeStruct((dim,), F32),
                jax.ShapeDtypeStruct((1, 128), F32),
                jax.ShapeDtypeStruct((tokens, vocab), BF16),
                jax.ShapeDtypeStruct((tokens, dim), BF16),
            ),
            in_specs=[any_spec, vmem_spec, any_spec, any_spec, any_spec],
            out_specs=(any_spec, vmem_spec, vmem_spec, any_spec, any_spec),
            scratch_shapes=[
                vm((tokens, dim), BF16),
                vm((tokens, dim), BF16),
                vm((vocab, dim), BF16),
                vm((tokens, kt), jnp.int32),
                vm((tokens, kt), F32),
                vm((tokens, vocab), F32),
                vm((tokens, 128), F32),
                vm((tokens, 128), F32),
                vm((tokens, 128), F32),
                vm((tokens, 128), F32),
                vm((vocab // 128 * rows_c, 128), F32),
                vm((tokens, vocab), BF16),
                vm((tokens, dim), F32),
                vm((tokens, dim), BF16),
                vm((tokens, dim), F32),
                vm((CHUNKS, half, dim), F32),
                vm((CHUNKS, 2, half // 4, dim), F32),
                vm((CHUNKS, 2, half // 8, dim), F32),
                vm((HALVES, 1, 2 * tokens // HALVES), F32),
                vm((HALVES, n_dev, 1, 2 * tokens // HALVES), F32),
                vm((1, dim + 128), F32),
                vm((n_dev, 1, dim + 128), F32),
                vm((8, dim), F32),
                vm((16, 128), F32),
                dma((vocab // VT,)),
                dma((3,)),
                dma((1 + 2 * CHUNKS,)),
                dma((HALVES, n_dev - 1)),
                dma((HALVES, n_dev - 1)),
                dma((n_dev - 1,)),
                dma((n_dev - 1,)),
                dma((CHUNKS, 2, 10)),
                dma((CHUNKS, 2, 10)),
            ],
            compiler_params=pltpu.CompilerParams(
                collective_id=0, has_side_effects=True, vmem_limit_bytes=67_043_328),
            name='fused_head',
        )(hidden, norm_gain, emb_block, teacher_ids, teacher_q)
        grad_block, dh, dw, loss = pl.pallas_call(
            table_kernel,
            in_specs=[any_spec, any_spec, any_spec, vmem_spec, vmem_spec],
            out_specs=(any_spec, any_spec, vmem_spec, vmem_spec),
            out_shape=(
                jax.ShapeDtypeStruct((vocab, dim), F32),
                jax.ShapeDtypeStruct((tokens, dim), BF16),
                jax.ShapeDtypeStruct((dim,), F32),
                jax.ShapeDtypeStruct((1, 128), F32),
            ),
            scratch_shapes=[
                vm((tokens, vocab), BF16),
                vm((tokens, dim), BF16),
                vm((SLOTS, TT, dim), F32),
                vm((tokens, dim), BF16),
                dma,
                dma((vocab // TT,)),
                dma((SLOTS, 2)),
                dma((2,)),
            ],
            compiler_params=pltpu.CompilerParams(vmem_limit_bytes=67_043_328),
            name='table_grad',
        )(dz, x_in, dh, dw, loss)
        return (loss[0, 0:1], dh, dw, grad_block)

    return jax.shard_map(local_step, mesh=mesh, in_specs=(P('dp', None), P(None), P('tp', None), P('dp', None), P('dp', None)), out_specs=(P('dp'), P('dp', None), P('dp'), P(('dp', 'tp'), None)), check_vma=False)
```

```python
import jax
import jax.numpy as jnp
from jax import lax
from jax.experimental import pallas as pl
from jax.experimental.pallas import tpu as pltpu
from jax.sharding import PartitionSpec as P

MESH = pl.DeviceIdType.MESH
F32 = jnp.float32
BF16 = jnp.bfloat16
NT = (((1,), (1,)), ((), ()))
TN = (((0,), (0,)), ((), ()))
CHUNKS = 4
HALVES = 2
VT = 512
SLOTS = 3
TT = 512
TOK = 32


def fused_kernel(n_dev, h_hbm, w_ref, e_hbm, ids_hbm, q_hbm,
                 dh_hbm, dw_ref, loss_ref, dz_hbm, x_hbm,
                 h_v, x_v, e_v, ids_v, q_v, z_v, mx_v, sm_v, lz_v, sn_v, qs_v, dz_v, dx_v, dh_v, g_v,
                 r0_v, r1_v, r2_v, st_send, st_recv, fin_send, fin_recv, dwacc_v, qz_v,
                 e_sem, in_sem, out_sem, st_ss, st_rs, fin_ss, fin_rs, ss, rs):
    tokens, dim = h_v.shape
    vocab = e_v.shape[0]
    rows_c = tokens // CHUNKS
    groups = vocab // 128
    half = rows_c // 2
    n_blk = vocab // VT
    me = lax.axis_index('tp')
    dp = lax.axis_index('dp')
    core = me % 2
    xc = (me // 2) % 2
    yc = me // 4
    sib = me + 1 - 2 * core
    xn = me + 2 - 4 * xc
    yn = me + 4 - 8 * yc
    base = me * vocab
    inv_tokens = 1.0 / tokens

    def al(value, mult):
        return pl.multiple_of(value, mult)

    h_copy = pltpu.make_async_copy(h_hbm, h_v, in_sem.at[0])
    ids_copy = pltpu.make_async_copy(ids_hbm, ids_v, in_sem.at[1])
    q_copy = pltpu.make_async_copy(q_hbm, q_v, in_sem.at[2])
    q_copy.start()
    h_copy.start()

    def e_copy(i):
        rows = pl.ds(al(i * VT, VT), VT)
        return pltpu.make_async_copy(e_hbm.at[rows], e_v.at[rows], e_sem.at[i])

    @pl.loop(0, n_blk)
    def _(i):
        e_copy(i).start()

    ids_copy.start()

    barrier = pltpu.get_barrier_semaphore()
    for i in range(1, n_dev):
        pl.semaphore_signal(barrier, inc=1, device_id=(dp, (me + i) % n_dev), device_id_type=MESH)

    q_copy.wait()

    @pl.loop(0, tokens // 64)
    def _(i):
        rows = pl.ds(al(i * 64, 64), 64)
        sn_v[rows, :] = jnp.broadcast_to(jnp.sum(q_v[rows, :], axis=1, keepdims=True), (64, 128))

    h_copy.wait()
    gain = w_ref[...].reshape(1, dim) + 1.0

    part = tokens // HALVES

    def norm(h):
        @pl.loop(0, part // 64)
        def _(i):
            rows = pl.ds(al(h * part + i * 64, 64), 64)
            acc = jnp.zeros((64, 128), F32)
            for k in range(dim // 128):
                hf = h_v[rows, 128 * k:128 * (k + 1)].astype(F32)
                acc = acc + hf * hf
            inv = lax.rsqrt(jnp.sum(acc, axis=1, keepdims=True) * (1.0 / dim) + 1e-6)
            inv = jnp.broadcast_to(inv, (64, 128))
            for k in range(dim // 128):
                hf = h_v[rows, 128 * k:128 * (k + 1)].astype(F32)
                x_v[rows, 128 * k:128 * (k + 1)] = (hf * inv * gain[:, 128 * k:128 * (k + 1)]).astype(BF16)

    mx_v[...] = jnp.full(mx_v.shape, -jnp.inf, F32)
    sm_v[...] = jnp.zeros(sm_v.shape, F32)

    def logits(h, first, last):
        rows = slice(h * part, (h + 1) * part)

        @pl.loop(first, last)
        def _(i):
            if h == 0:
                e_copy(i).wait()
            zb = lax.dot_general(x_v[rows, :], e_v[pl.ds(al(i * VT, VT), VT), :], NT, preferred_element_type=F32)
            z_v[rows, pl.ds(al(i * VT, VT), VT)] = zb
            old = mx_v[rows, :]
            new = old
            for k in range(VT // 128):
                new = jnp.maximum(new, zb[:, 128 * k:128 * (k + 1)])
            total = sm_v[rows, :] * jnp.exp(old - new)
            for k in range(VT // 128):
                total = total + jnp.exp(zb[:, 128 * k:128 * (k + 1)] - new)
            mx_v[rows, :] = new
            sm_v[rows, :] = total

    def gather_copies(src, dst, s_sem, r_sem):
        out = []
        for i in range(1, n_dev):
            out.append(pltpu.make_async_remote_copy(
                src_ref=src, dst_ref=dst.at[me], send_sem=s_sem.at[i - 1], recv_sem=r_sem.at[i - 1],
                device_id=(dp, (me + i) % n_dev), device_id_type=MESH))
        return out

    st_copies = [gather_copies(st_send.at[h], st_recv.at[h], st_ss.at[h], st_rs.at[h]) for h in range(HALVES)]

    def send_stats(h):
        for b in range(part // 128):
            span = slice(h * part + 128 * b, h * part + 128 * (b + 1))
            peaks = mx_v[span, :].T
            peak = jnp.max(peaks, axis=0, keepdims=True)
            st_send[h, :, 128 * b:128 * (b + 1)] = peak
            st_send[h, :, part + 128 * b:part + 128 * (b + 1)] = jnp.sum(
                sm_v[span, :].T * jnp.exp(peaks - peak), axis=0, keepdims=True)
        st_recv[h, me] = st_send[h]
        if h == 0:
            pl.semaphore_wait(barrier, n_dev - 1)
        for copy in st_copies[h]:
            copy.start()

    def take_stats(h):
        for copy in st_copies[h]:
            copy.wait_recv()
        peak = st_recv[h, 0][:, 0:part]
        for d in range(1, n_dev):
            peak = jnp.maximum(peak, st_recv[h, d][:, 0:part])
        total = jnp.zeros((1, part), F32)
        for d in range(n_dev):
            total = total + st_recv[h, d][:, part:2 * part] * jnp.exp(st_recv[h, d][:, 0:part] - peak)
        log_z = peak + jnp.log(total)
        for b in range(part // 128):
            lz_v[h * part + 128 * b:h * part + 128 * (b + 1), :] = jnp.broadcast_to(
                log_z[:, 128 * b:128 * (b + 1)], (128, 128)).T

    norm(0)
    logits(0, 0, n_blk)
    send_stats(0)
    norm(1)
    x_copy = pltpu.make_async_copy(x_v, x_hbm, out_sem.at[0])
    x_copy.start()
    ids_copy.wait()

    iota_hi = lax.broadcasted_iota(jnp.int32, (groups, 256), 0)
    iota_lo = lax.broadcasted_iota(jnp.int32, (128, 256), 0)

    def build_q(c, p):
        @pl.loop(p * rows_c // TOK // 2, (p + 1) * rows_c // TOK // 2)
        def _(t):
            for u in range(TOK):
                local = t * TOK + u
                row = pl.ds(c * rows_c + local, 1)
                ids = ids_v[row, :] - base
                qv = q_v[row, :]
                q_a = qv.astype(BF16).astype(F32)
                rest = qv - q_a
                q_b = rest.astype(BF16).astype(F32)
                q_c = rest - q_b
                hot_hi = lax.shift_right_arithmetic(ids, 7) == iota_hi
                hot_lo = jnp.where((ids & 127) == iota_lo, 1.0, 0.0).astype(BF16)
                parts = [jnp.where(hot_hi, part, 0.0).astype(BF16) for part in (q_a, q_b, q_c)]
                res = lax.dot_general(jnp.concatenate(parts, axis=0), hot_lo, NT, preferred_element_type=F32)
                dense = res[0:groups] + res[groups:2 * groups] + res[2 * groups:3 * groups]
                qs_v[pl.ds(local, groups, stride=rows_c), :] = dense

    def make_dz(c):
        @pl.loop(0, rows_c // 16)
        def _(i):
            off = al(i * 16, 16)
            rows = pl.ds(al(c * rows_c + off, 16), 16)
            lz = lz_v[rows, :]
            sn = sn_v[rows, :]
            acc = jnp.zeros((16, 128), F32)
            for k in range(groups):
                zz = z_v[rows, 128 * k:128 * (k + 1)]
                qq = qs_v[pl.ds(al(k * rows_c + off, 16), 16), :]
                acc = acc + qq * zz
                d = (jnp.exp(zz - lz) * sn - qq) * inv_tokens
                dz_v[rows, 128 * k:128 * (k + 1)] = d.astype(BF16)
            qz_v[...] = qz_v[...] + acc

    def make_dx(c, p):
        rows = slice(c * rows_c, (c + 1) * rows_c)

        @pl.loop(p * dim // 256 // 2, (p + 1) * dim // 256 // 2)
        def _(j):
            cols = pl.ds(al(j * 256, 256), 256)
            dx_v[rows, cols] = jnp.dot(dz_v[rows, :], e_v[:, cols], preferred_element_type=F32)

    q8 = half // 8
    q4 = half // 4
    q2 = half // 2

    wide = dim // 2
    cut = (slice(0, wide), slice(wide, 2 * wide))

    def rcopy(src, dst, c, p, slot, dev):
        return pltpu.make_async_remote_copy(
            src_ref=src, dst_ref=dst, send_sem=ss.at[c, p, slot], recv_sem=rs.at[c, p, slot],
            device_id=(dp, dev), device_id_type=MESH)

    def mine(c):
        return c * rows_c + half * core

    sent = []

    def go(*copies):
        for copy in copies:
            copy.start()
            sent.append(copy)

    def dx_at(start, size, p):
        return dx_v.at[pl.ds(al(start, size), size), cut[p]]

    def g_at(start, size, p):
        return g_v.at[pl.ds(al(start, size), size), cut[p]]

    def s0(c, p):
        return rcopy(dx_at(c * rows_c + half * (1 - core), half, p), r0_v.at[c, :, cut[p]], c, p, 0, sib)

    def s1(c, p):
        a = rcopy(dx_at(mine(c) + q4 * (1 - xc), q4, p), r1_v.at[c, 0, :, cut[p]], c, p, 1, xn)
        b = rcopy(dx_at(mine(c) + q2 + q4 * (1 - yc), q4, p), r1_v.at[c, 1, :, cut[p]], c, p, 2, yn)
        return a, b

    def s2(c, p):
        a = rcopy(dx_at(mine(c) + q4 * xc + q8 * (1 - yc), q8, p), r2_v.at[c, 0, :, cut[p]], c, p, 3, yn)
        b = rcopy(dx_at(mine(c) + q2 + q4 * yc + q8 * (1 - xc), q8, p), r2_v.at[c, 1, :, cut[p]], c, p, 4, xn)
        return a, b

    def s3(c, p):
        a = g_at(mine(c) + q4 * xc + q8 * yc, q8, p)
        b = g_at(mine(c) + q2 + q4 * yc + q8 * xc, q8, p)
        return rcopy(a, a, c, p, 5, yn), rcopy(b, b, c, p, 6, xn)

    def s4(c, p):
        a = g_at(mine(c) + q4 * xc, q4, p)
        b = g_at(mine(c) + q2 + q4 * yc, q4, p)
        return rcopy(a, a, c, p, 7, xn), rcopy(b, b, c, p, 8, yn)

    def s5(c, p):
        a = g_at(mine(c), half, p)
        return rcopy(a, a, c, p, 9, sib)

    def f0(c, p):
        go(s0(c, p))

    def f1(c, p):
        s0(c, p).wait_recv()

        @pl.loop(0, half // 8)
        def _(i):
            rows = pl.ds(al(mine(c) + 8 * i, 8), 8)
            dx_v[rows, cut[p]] = dx_v[rows, cut[p]] + r0_v[c, pl.ds(al(8 * i, 8), 8), cut[p]]
        go(*s1(c, p))

    def f2(c, p):
        for copy in s1(c, p):
            copy.wait_recv()
        for k, start in ((0, mine(c) + q4 * xc), (1, mine(c) + q2 + q4 * yc)):
            rows = pl.ds(al(start, q4), q4)
            dx_v[rows, cut[p]] = dx_v[rows, cut[p]] + r1_v[c, k, :, cut[p]]
        go(*s2(c, p))

    def norm_back(c, k, block, side):
        rows16 = pl.ds(al(block, 16), 16)
        rows = pl.ds(al(block + q8 * side, q8), q8)
        hb = h_v[rows16, :].astype(F32)
        hf = jnp.where(side == 0, hb[0:8, :], hb[8:16, :])
        grad = dx_v[rows, :] + r2_v[c, k]
        inv = lax.rsqrt(jnp.mean(hf * hf, axis=1, keepdims=True) + 1e-6)
        scaled = grad * gain
        mean = jnp.sum(scaled * hf, axis=1, keepdims=True) * (1.0 / dim)
        g_v[rows, :] = scaled * inv - hf * (inv * inv * inv * mean)
        dwacc_v[...] = dwacc_v[...] + grad * hf * inv

    def f3(c):
        for p in range(2):
            for copy in s2(c, p):
                copy.wait_recv()
        norm_back(c, 0, mine(c) + q4 * xc, yc)
        norm_back(c, 1, mine(c) + q2 + q4 * yc, xc)
        for p in range(2):
            go(*s3(c, p))

    def f4(c, p):
        for copy in s3(c, p):
            copy.wait_recv()
        go(*s4(c, p))

    def f5(c, p):
        for copy in s4(c, p):
            copy.wait_recv()
        go(s5(c, p))

    def rows_of(c):
        return slice(c * rows_c, (c + 1) * rows_c)

    def dh_copy(c):
        return pltpu.make_async_copy(dh_v.at[rows_of(c)], dh_hbm.at[rows_of(c)], out_sem.at[1 + c])

    def dz_copy(c):
        return pltpu.make_async_copy(dz_v.at[rows_of(c)], dz_hbm.at[rows_of(c)], out_sem.at[1 + CHUNKS + c])

    def f6(c):
        for p in range(2):
            s5(c, p).wait_recv()

        @pl.loop(0, rows_c // 16)
        def _(i):
            rows = pl.ds(al(c * rows_c + 16 * i, 16), 16)
            dh_v[rows, :] = g_v[rows, :].astype(BF16)
        dh_copy(c).start()

    dwacc_v[...] = jnp.zeros(dwacc_v.shape, F32)
    qz_v[...] = jnp.zeros(qz_v.shape, F32)

    def finish_dz(c):
        make_dz(c)
        dz_copy(c).start()

    quarter = n_blk // 4
    build_q(0, 0)
    build_q(0, 1)
    take_stats(0)
    finish_dz(0)
    make_dx(0, 0)
    f0(0, 0)
    make_dx(0, 1)
    f0(0, 1)
    build_q(1, 0)
    f1(0, 0)
    build_q(1, 1)
    f1(0, 1)
    finish_dz(1)
    make_dx(1, 0)
    f0(1, 0)
    make_dx(1, 1)
    f0(1, 1)
    f2(0, 0)
    logits(1, 0, quarter)
    f1(1, 0)
    f2(0, 1)
    logits(1, quarter, 2 * quarter)
    f1(1, 1)
    logits(1, 2 * quarter, n_blk)
    send_stats(1)
    f3(0)
    f2(1, 0)
    build_q(2, 0)
    f2(1, 1)
    build_q(2, 1)
    take_stats(1)
    finish_dz(2)
    make_dx(2, 0)
    f0(2, 0)
    f4(0, 0)
    f4(0, 1)
    f3(1)
    make_dx(2, 1)
    f0(2, 1)
    build_q(3, 0)
    f1(2, 0)
    build_q(3, 1)
    f1(2, 1)
    f4(1, 0)
    f4(1, 1)
    finish_dz(3)
    make_dx(3, 0)
    f0(3, 0)
    f5(0, 0)
    f5(0, 1)
    make_dx(3, 1)
    f0(3, 1)
    f1(3, 0)
    f2(2, 0)
    f2(2, 1)
    f5(1, 0)
    f5(1, 1)
    f1(3, 1)
    f6(0)
    f2(3, 0)
    f3(2)
    f2(3, 1)
    f6(1)
    f4(2, 0)
    f4(2, 1)
    f3(3)
    fin_send[:, 0:dim] = jnp.sum(dwacc_v[...], axis=0, keepdims=True)
    fin_send[:, dim:dim + 128] = jnp.sum(qz_v[...], axis=0, keepdims=True)
    fin_recv[me] = fin_send[...]
    fin_copies = gather_copies(fin_send, fin_recv, fin_ss, fin_rs)
    for copy in fin_copies:
        copy.start()
    f5(2, 0)
    f5(2, 1)
    f4(3, 0)
    f4(3, 1)
    f6(2)
    f5(3, 0)
    f5(3, 1)

    for copy in fin_copies:
        copy.wait_recv()
    fin = fin_recv[0]
    for d in range(1, n_dev):
        fin = fin + fin_recv[d]
    dw_ref[...] = fin[:, 0:dim].reshape(dim)
    weighted = jnp.sum(lz_v[...] * sn_v[...], axis=0, keepdims=True)
    loss_ref[...] = (weighted - jnp.sum(fin[:, dim:dim + 128])) * inv_tokens
    f6(3)

    for copy in st_copies[0] + st_copies[1] + sent + fin_copies:
        copy.wait_send()
    x_copy.wait()
    for c in range(CHUNKS):
        dz_copy(c).wait()
        dh_copy(c).wait()


def table_kernel(dz_hbm, x_hbm, dh_hbm, dw_ref, loss_ref, out_hbm, dh_out, dw_out, loss_out,
                 dz_v, x_v, o_v, dh_v, x_sem, dz_sem, out_sem, dh_sem):
    n_blk = out_hbm.shape[0] // TT
    half = out_hbm.shape[1] // 2
    cuts = (slice(0, half), slice(half, 2 * half))

    def dz_copy(i):
        cols = pl.ds(pl.multiple_of(i * TT, TT), TT)
        return pltpu.make_async_copy(dz_hbm.at[:, cols], dz_v.at[:, cols], dz_sem.at[i])

    def out_copy(i, k):
        slot = lax.rem(i, SLOTS)
        rows = pl.ds(pl.multiple_of(i * TT, TT), TT)
        return pltpu.make_async_copy(o_v.at[slot, :, cuts[k]], out_hbm.at[rows, cuts[k]], out_sem.at[slot, k])

    x_copy = pltpu.make_async_copy(x_hbm, x_v, x_sem)
    x_copy.start()

    @pl.loop(0, n_blk)
    def _(i):
        dz_copy(i).start()

    dh_in = pltpu.make_async_copy(dh_hbm, dh_v, dh_sem.at[0])
    dh_put = pltpu.make_async_copy(dh_v, dh_out, dh_sem.at[1])
    dh_in.start()
    dw_out[...] = dw_ref[...]
    loss_out[...] = loss_ref[...]
    x_copy.wait()

    @pl.loop(0, n_blk)
    def _(i):
        dz_copy(i).wait()

        @pl.when(i >= SLOTS)
        def _():
            out_copy(i - SLOTS, 0).wait()
            out_copy(i - SLOTS, 1).wait()

        cols = pl.ds(pl.multiple_of(i * TT, TT), TT)
        for k in range(2):
            o_v[lax.rem(i, SLOTS), :, cuts[k]] = lax.dot_general(
                dz_v[:, cols], x_v[:, cuts[k]], TN, preferred_element_type=F32)
            out_copy(i, k).start()

        @pl.when(i == 1)
        def _():
            dh_in.wait()
            dh_put.start()

    for i in range(n_blk - SLOTS, n_blk):
        out_copy(i, 0).wait()
        out_copy(i, 1).wait()
    dh_put.wait()


def solution(mesh):
    n_dev = mesh.shape['tp']

    def local_step(hidden, norm_gain, emb_block, teacher_ids, teacher_q):
        tokens, dim = hidden.shape
        vocab = emb_block.shape[0]
        rows_c = tokens // CHUNKS
        half = rows_c // 2
        kt = teacher_ids.shape[1]
        any_spec = pl.BlockSpec(memory_space=pl.ANY)
        vmem_spec = pl.BlockSpec(memory_space=pltpu.VMEM)
        vm = pltpu.VMEM
        dma = pltpu.SemaphoreType.DMA
        dh, dw, loss, dz, x_in = pl.pallas_call(
            lambda *refs: fused_kernel(n_dev, *refs),
            out_shape=(
                jax.ShapeDtypeStruct((tokens, dim), BF16),
                jax.ShapeDtypeStruct((dim,), F32),
                jax.ShapeDtypeStruct((1, 128), F32),
                jax.ShapeDtypeStruct((tokens, vocab), BF16),
                jax.ShapeDtypeStruct((tokens, dim), BF16),
            ),
            in_specs=[any_spec, vmem_spec, any_spec, any_spec, any_spec],
            out_specs=(any_spec, vmem_spec, vmem_spec, any_spec, any_spec),
            scratch_shapes=[
                vm((tokens, dim), BF16),
                vm((tokens, dim), BF16),
                vm((vocab, dim), BF16),
                vm((tokens, kt), jnp.int32),
                vm((tokens, kt), F32),
                vm((tokens, vocab), F32),
                vm((tokens, 128), F32),
                vm((tokens, 128), F32),
                vm((tokens, 128), F32),
                vm((tokens, 128), F32),
                vm((vocab // 128 * rows_c, 128), F32),
                vm((tokens, vocab), BF16),
                vm((tokens, dim), F32),
                vm((tokens, dim), BF16),
                vm((tokens, dim), F32),
                vm((CHUNKS, half, dim), F32),
                vm((CHUNKS, 2, half // 4, dim), F32),
                vm((CHUNKS, 2, half // 8, dim), F32),
                vm((HALVES, 1, 2 * tokens // HALVES), F32),
                vm((HALVES, n_dev, 1, 2 * tokens // HALVES), F32),
                vm((1, dim + 128), F32),
                vm((n_dev, 1, dim + 128), F32),
                vm((8, dim), F32),
                vm((16, 128), F32),
                dma((vocab // VT,)),
                dma((3,)),
                dma((1 + 2 * CHUNKS,)),
                dma((HALVES, n_dev - 1)),
                dma((HALVES, n_dev - 1)),
                dma((n_dev - 1,)),
                dma((n_dev - 1,)),
                dma((CHUNKS, 2, 10)),
                dma((CHUNKS, 2, 10)),
            ],
            compiler_params=pltpu.CompilerParams(
                collective_id=0, has_side_effects=True, vmem_limit_bytes=67_043_328),
            name='fused_head',
        )(hidden, norm_gain, emb_block, teacher_ids, teacher_q)
        grad_block, dh, dw, loss = pl.pallas_call(
            table_kernel,
            in_specs=[any_spec, any_spec, any_spec, vmem_spec, vmem_spec],
            out_specs=(any_spec, any_spec, vmem_spec, vmem_spec),
            out_shape=(
                jax.ShapeDtypeStruct((vocab, dim), F32),
                jax.ShapeDtypeStruct((tokens, dim), BF16),
                jax.ShapeDtypeStruct((dim,), F32),
                jax.ShapeDtypeStruct((1, 128), F32),
            ),
            scratch_shapes=[
                vm((tokens, vocab), BF16),
                vm((tokens, dim), BF16),
                vm((SLOTS, TT, dim), F32),
                vm((tokens, dim), BF16),
                dma,
                dma((vocab // TT,)),
                dma((SLOTS, 2)),
                dma((2,)),
            ],
            compiler_params=pltpu.CompilerParams(vmem_limit_bytes=67_043_328),
            name='table_grad',
        )(dz, x_in, dh, dw, loss)
        return (loss[0, 0:1], dh, dw, grad_block)

    return jax.shard_map(local_step, mesh=mesh, in_specs=(P('dp', None), P(None), P('tp', None), P('dp', None), P('dp', None)), out_specs=(P('dp'), P('dp', None), P('dp'), P(('dp', 'tp'), None)), check_vma=False)
```

```python
import jax
import jax.numpy as jnp
from jax import lax
from jax.experimental import pallas as pl
from jax.experimental.pallas import tpu as pltpu
from jax.sharding import PartitionSpec as P

MESH = pl.DeviceIdType.MESH
F32 = jnp.float32
BF16 = jnp.bfloat16
NT = (((1,), (1,)), ((), ()))
TN = (((0,), (0,)), ((), ()))
CHUNKS = 4
HALVES = 2
VT = 512
SLOTS = 3
TT = 512
TOK = 32


def fused_kernel(n_dev, h_hbm, w_ref, e_hbm, ids_hbm, q_hbm,
                 dh_hbm, dw_ref, loss_ref, dz_hbm, x_hbm,
                 h_v, x_v, e_v, ids_v, q_v, z_v, mx_v, sm_v, lz_v, sn_v, qs_v, dz_v, dx_v, dh_v, g_v,
                 r0_v, r1_v, r2_v, st_send, st_recv, fin_send, fin_recv, dwacc_v, qz_v,
                 e_sem, in_sem, out_sem, st_ss, st_rs, fin_ss, fin_rs, ss, rs):
    tokens, dim = h_v.shape
    vocab = e_v.shape[0]
    rows_c = tokens // CHUNKS
    groups = vocab // 128
    half = rows_c // 2
    n_blk = vocab // VT
    me = lax.axis_index('tp')
    dp = lax.axis_index('dp')
    core = me % 2
    xc = (me // 2) % 2
    yc = me // 4
    sib = me + 1 - 2 * core
    xn = me + 2 - 4 * xc
    yn = me + 4 - 8 * yc
    base = me * vocab
    inv_tokens = 1.0 / tokens

    def al(value, mult):
        return pl.multiple_of(value, mult)

    part = tokens // HALVES

    def h_copy(h):
        rows = slice(h * part, (h + 1) * part)
        return pltpu.make_async_copy(h_hbm.at[rows], h_v.at[rows], in_sem.at[3 * h])

    ids_copy = pltpu.make_async_copy(ids_hbm, ids_v, in_sem.at[1])
    q_copy = pltpu.make_async_copy(q_hbm, q_v, in_sem.at[2])
    q_copy.start()
    h_copy(0).start()

    def e_copy(i):
        rows = pl.ds(al(i * VT, VT), VT)
        return pltpu.make_async_copy(e_hbm.at[rows], e_v.at[rows], e_sem.at[i])

    @pl.loop(0, n_blk)
    def _(i):
        e_copy(i).start()

    h_copy(1).start()
    ids_copy.start()

    barrier = pltpu.get_barrier_semaphore()
    for i in range(1, n_dev):
        pl.semaphore_signal(barrier, inc=1, device_id=(dp, (me + i) % n_dev), device_id_type=MESH)

    q_copy.wait()

    @pl.loop(0, tokens // 64)
    def _(i):
        rows = pl.ds(al(i * 64, 64), 64)
        sn_v[rows, :] = jnp.broadcast_to(jnp.sum(q_v[rows, :], axis=1, keepdims=True), (64, 128))

    gain = w_ref[...].reshape(1, dim) + 1.0

    def norm(h):
        h_copy(h).wait()

        @pl.loop(0, part // 64)
        def _(i):
            rows = pl.ds(al(h * part + i * 64, 64), 64)
            acc = jnp.zeros((64, 128), F32)
            for k in range(dim // 128):
                hf = h_v[rows, 128 * k:128 * (k + 1)].astype(F32)
                acc = acc + hf * hf
            inv = lax.rsqrt(jnp.sum(acc, axis=1, keepdims=True) * (1.0 / dim) + 1e-6)
            inv = jnp.broadcast_to(inv, (64, 128))
            for k in range(dim // 128):
                hf = h_v[rows, 128 * k:128 * (k + 1)].astype(F32)
                x_v[rows, 128 * k:128 * (k + 1)] = (hf * inv * gain[:, 128 * k:128 * (k + 1)]).astype(BF16)

    mx_v[...] = jnp.full(mx_v.shape, -jnp.inf, F32)
    sm_v[...] = jnp.zeros(sm_v.shape, F32)

    def logits(h, first, last):
        rows = slice(h * part, (h + 1) * part)

        @pl.loop(first, last)
        def _(i):
            if h == 0:
                e_copy(i).wait()
            zb = lax.dot_general(x_v[rows, :], e_v[pl.ds(al(i * VT, VT), VT), :], NT, preferred_element_type=F32)
            z_v[rows, pl.ds(al(i * VT, VT), VT)] = zb
            old = mx_v[rows, :]
            new = old
            for k in range(VT // 128):
                new = jnp.maximum(new, zb[:, 128 * k:128 * (k + 1)])
            total = sm_v[rows, :] * jnp.exp(old - new)
            for k in range(VT // 128):
                total = total + jnp.exp(zb[:, 128 * k:128 * (k + 1)] - new)
            mx_v[rows, :] = new
            sm_v[rows, :] = total

    def gather_copies(src, dst, s_sem, r_sem):
        out = []
        for i in range(1, n_dev):
            out.append(pltpu.make_async_remote_copy(
                src_ref=src, dst_ref=dst.at[me], send_sem=s_sem.at[i - 1], recv_sem=r_sem.at[i - 1],
                device_id=(dp, (me + i) % n_dev), device_id_type=MESH))
        return out

    st_copies = [gather_copies(st_send.at[h], st_recv.at[h], st_ss.at[h], st_rs.at[h]) for h in range(HALVES)]

    def send_stats(h):
        for b in range(part // 128):
            span = slice(h * part + 128 * b, h * part + 128 * (b + 1))
            peaks = mx_v[span, :].T
            peak = jnp.max(peaks, axis=0, keepdims=True)
            st_send[h, :, 128 * b:128 * (b + 1)] = peak
            st_send[h, :, part + 128 * b:part + 128 * (b + 1)] = jnp.sum(
                sm_v[span, :].T * jnp.exp(peaks - peak), axis=0, keepdims=True)
        st_recv[h, me] = st_send[h]
        if h == 0:
            pl.semaphore_wait(barrier, n_dev - 1)
        for copy in st_copies[h]:
            copy.start()

    def take_stats(h):
        for copy in st_copies[h]:
            copy.wait_recv()
        peak = st_recv[h, 0][:, 0:part]
        for d in range(1, n_dev):
            peak = jnp.maximum(peak, st_recv[h, d][:, 0:part])
        total = jnp.zeros((1, part), F32)
        for d in range(n_dev):
            total = total + st_recv[h, d][:, part:2 * part] * jnp.exp(st_recv[h, d][:, 0:part] - peak)
        log_z = peak + jnp.log(total)
        for b in range(part // 128):
            lz_v[h * part + 128 * b:h * part + 128 * (b + 1), :] = jnp.broadcast_to(
                log_z[:, 128 * b:128 * (b + 1)], (128, 128)).T

    iota_hi = lax.broadcasted_iota(jnp.int32, (groups, 256), 0)
    iota_lo = lax.broadcasted_iota(jnp.int32, (128, 256), 0)

    def build_q(c, p):
        @pl.loop(p * rows_c // TOK // 2, (p + 1) * rows_c // TOK // 2)
        def _(t):
            for u in range(TOK):
                local = t * TOK + u
                row = pl.ds(c * rows_c + local, 1)
                ids = ids_v[row, :] - base
                qv = q_v[row, :]
                q_a = qv.astype(BF16).astype(F32)
                rest = qv - q_a
                q_b = rest.astype(BF16).astype(F32)
                q_c = rest - q_b
                hot_hi = lax.shift_right_arithmetic(ids, 7) == iota_hi
                hot_lo = jnp.where((ids & 127) == iota_lo, 1.0, 0.0).astype(BF16)
                parts = [jnp.where(hot_hi, part, 0.0).astype(BF16) for part in (q_a, q_b, q_c)]
                res = lax.dot_general(jnp.concatenate(parts, axis=0), hot_lo, NT, preferred_element_type=F32)
                dense = res[0:groups] + res[groups:2 * groups] + res[2 * groups:3 * groups]
                qs_v[pl.ds(local, groups, stride=rows_c), :] = dense

    def make_dz(c):
        @pl.loop(0, rows_c // 16)
        def _(i):
            off = al(i * 16, 16)
            rows = pl.ds(al(c * rows_c + off, 16), 16)
            lz = lz_v[rows, :]
            sn = sn_v[rows, :]
            acc = jnp.zeros((16, 128), F32)
            for k in range(groups):
                zz = z_v[rows, 128 * k:128 * (k + 1)]
                qq = qs_v[pl.ds(al(k * rows_c + off, 16), 16), :]
                acc = acc + qq * zz
                d = (jnp.exp(zz - lz) * sn - qq) * inv_tokens
                dz_v[rows, 128 * k:128 * (k + 1)] = d.astype(BF16)
            qz_v[...] = qz_v[...] + acc

    def make_dx(c, p):
        rows = slice(c * rows_c, (c + 1) * rows_c)

        @pl.loop(p * dim // 256 // 2, (p + 1) * dim // 256 // 2)
        def _(j):
            cols = pl.ds(al(j * 256, 256), 256)
            dx_v[rows, cols] = jnp.dot(dz_v[rows, :], e_v[:, cols], preferred_element_type=F32)

    q8 = half // 8
    q4 = half // 4
    q2 = half // 2

    wide = dim // 2
    cut = (slice(0, wide), slice(wide, 2 * wide))

    def rcopy(src, dst, c, p, slot, dev):
        return pltpu.make_async_remote_copy(
            src_ref=src, dst_ref=dst, send_sem=ss.at[c, p, slot], recv_sem=rs.at[c, p, slot],
            device_id=(dp, dev), device_id_type=MESH)

    def mine(c):
        return c * rows_c + half * core

    sent = []

    def go(*copies):
        for copy in copies:
            copy.start()
            sent.append(copy)

    def dx_at(start, size, p):
        return dx_v.at[pl.ds(al(start, size), size), cut[p]]

    def g_at(start, size, p):
        return g_v.at[pl.ds(al(start, size), size), cut[p]]

    def s0(c, p):
        return rcopy(dx_at(c * rows_c + half * (1 - core), half, p), r0_v.at[c, :, cut[p]], c, p, 0, sib)

    def s1(c, p):
        a = rcopy(dx_at(mine(c) + q4 * (1 - xc), q4, p), r1_v.at[c, 0, :, cut[p]], c, p, 1, xn)
        b = rcopy(dx_at(mine(c) + q2 + q4 * (1 - yc), q4, p), r1_v.at[c, 1, :, cut[p]], c, p, 2, yn)
        return a, b

    def s2(c, p):
        a = rcopy(dx_at(mine(c) + q4 * xc + q8 * (1 - yc), q8, p), r2_v.at[c, 0, :, cut[p]], c, p, 3, yn)
        b = rcopy(dx_at(mine(c) + q2 + q4 * yc + q8 * (1 - xc), q8, p), r2_v.at[c, 1, :, cut[p]], c, p, 4, xn)
        return a, b

    def s3(c, p):
        a = g_at(mine(c) + q4 * xc + q8 * yc, q8, p)
        b = g_at(mine(c) + q2 + q4 * yc + q8 * xc, q8, p)
        return rcopy(a, a, c, p, 5, yn), rcopy(b, b, c, p, 6, xn)

    def s4(c, p):
        a = g_at(mine(c) + q4 * xc, q4, p)
        b = g_at(mine(c) + q2 + q4 * yc, q4, p)
        return rcopy(a, a, c, p, 7, xn), rcopy(b, b, c, p, 8, yn)

    def s5(c, p):
        a = g_at(mine(c), half, p)
        return rcopy(a, a, c, p, 9, sib)

    def f0(c, p):
        go(s0(c, p))

    def f1(c, p):
        s0(c, p).wait_recv()

        @pl.loop(0, half // 8)
        def _(i):
            rows = pl.ds(al(mine(c) + 8 * i, 8), 8)
            dx_v[rows, cut[p]] = dx_v[rows, cut[p]] + r0_v[c, pl.ds(al(8 * i, 8), 8), cut[p]]
        go(*s1(c, p))

    def f2(c, p):
        for copy in s1(c, p):
            copy.wait_recv()
        for k, start in ((0, mine(c) + q4 * xc), (1, mine(c) + q2 + q4 * yc)):
            rows = pl.ds(al(start, q4), q4)
            dx_v[rows, cut[p]] = dx_v[rows, cut[p]] + r1_v[c, k, :, cut[p]]
        go(*s2(c, p))

    def norm_back(c, k, block, side):
        rows16 = pl.ds(al(block, 16), 16)
        rows = pl.ds(al(block + q8 * side, q8), q8)
        hb = h_v[rows16, :].astype(F32)
        hf = jnp.where(side == 0, hb[0:8, :], hb[8:16, :])
        grad = dx_v[rows, :] + r2_v[c, k]
        inv = lax.rsqrt(jnp.mean(hf * hf, axis=1, keepdims=True) + 1e-6)
        scaled = grad * gain
        mean = jnp.sum(scaled * hf, axis=1, keepdims=True) * (1.0 / dim)
        g_v[rows, :] = scaled * inv - hf * (inv * inv * inv * mean)
        dwacc_v[...] = dwacc_v[...] + grad * hf * inv

    def f3(c):
        for p in range(2):
            for copy in s2(c, p):
                copy.wait_recv()
        norm_back(c, 0, mine(c) + q4 * xc, yc)
        norm_back(c, 1, mine(c) + q2 + q4 * yc, xc)
        for p in range(2):
            go(*s3(c, p))

    def f4(c, p):
        for copy in s3(c, p):
            copy.wait_recv()
        go(*s4(c, p))

    def f5(c, p):
        for copy in s4(c, p):
            copy.wait_recv()
        go(s5(c, p))

    def rows_of(c):
        return slice(c * rows_c, (c + 1) * rows_c)

    def dh_copy(c):
        return pltpu.make_async_copy(dh_v.at[rows_of(c)], dh_hbm.at[rows_of(c)], out_sem.at[1 + c])

    def dz_copy(c):
        return pltpu.make_async_copy(dz_v.at[rows_of(c)], dz_hbm.at[rows_of(c)], out_sem.at[1 + CHUNKS + c])

    def f6(c):
        for p in range(2):
            s5(c, p).wait_recv()

        @pl.loop(0, rows_c // 16)
        def _(i):
            rows = pl.ds(al(c * rows_c + 16 * i, 16), 16)
            dh_v[rows, :] = g_v[rows, :].astype(BF16)
        dh_copy(c).start()

    dwacc_v[...] = jnp.zeros(dwacc_v.shape, F32)
    qz_v[...] = jnp.zeros(qz_v.shape, F32)

    def finish_dz(c):
        make_dz(c)
        dz_copy(c).start()

    quarter = n_blk // 4
    norm(0)
    logits(0, 0, n_blk)
    send_stats(0)
    norm(1)
    x_copy = pltpu.make_async_copy(x_v, x_hbm, out_sem.at[0])
    x_copy.start()
    ids_copy.wait()
    build_q(0, 0)
    build_q(0, 1)
    take_stats(0)
    finish_dz(0)
    make_dx(0, 0)
    f0(0, 0)
    make_dx(0, 1)
    f0(0, 1)
    build_q(1, 0)
    f1(0, 0)
    build_q(1, 1)
    f1(0, 1)
    finish_dz(1)
    make_dx(1, 1)
    f0(1, 1)
    make_dx(1, 0)
    f2(0, 0)
    f0(1, 0)
    f2(0, 1)
    logits(1, 0, quarter)
    f1(1, 1)
    logits(1, quarter, 2 * quarter)
    f1(1, 0)
    logits(1, 2 * quarter, 3 * quarter)
    f3(0)
    logits(1, 3 * quarter, n_blk)
    send_stats(1)
    f2(1, 1)
    build_q(2, 0)
    f2(1, 0)
    f4(0, 0)
    build_q(2, 1)
    f4(0, 1)
    take_stats(1)
    finish_dz(2)
    make_dx(2, 0)
    f0(2, 0)
    f3(1)
    make_dx(2, 1)
    f0(2, 1)
    f1(2, 0)
    build_q(3, 0)
    f4(1, 0)
    build_q(3, 1)
    finish_dz(3)
    f4(1, 1)
    f1(2, 1)
    make_dx(3, 0)
    f0(3, 0)
    f5(0, 1)
    f2(2, 0)
    make_dx(3, 1)
    f0(3, 1)
    f1(3, 0)
    f2(2, 1)
    f1(3, 1)
    f2(3, 0)
    f3(2)
    f5(0, 0)
    f2(3, 1)
    f4(2, 0)
    f3(3)
    f5(1, 0)
    f4(2, 1)
    f5(2, 0)
    fin_send[:, 0:dim] = jnp.sum(dwacc_v[...], axis=0, keepdims=True)
    fin_send[:, dim:dim + 128] = jnp.sum(qz_v[...], axis=0, keepdims=True)
    fin_recv[me] = fin_send[...]
    fin_copies = gather_copies(fin_send, fin_recv, fin_ss, fin_rs)
    for copy in fin_copies:
        copy.start()
    f4(3, 0)
    f4(3, 1)
    f6(0)
    f5(1, 1)
    f5(2, 1)
    f5(3, 0)
    f5(3, 1)
    f6(2)
    f6(1)

    for copy in fin_copies:
        copy.wait_recv()
    fin = fin_recv[0]
    for d in range(1, n_dev):
        fin = fin + fin_recv[d]
    dw_ref[...] = fin[:, 0:dim].reshape(dim)
    weighted = jnp.sum(lz_v[...] * sn_v[...], axis=0, keepdims=True)
    loss_ref[...] = (weighted - jnp.sum(fin[:, dim:dim + 128])) * inv_tokens
    f6(3)

    for copy in st_copies[0] + st_copies[1] + sent + fin_copies:
        copy.wait_send()
    x_copy.wait()
    for c in range(CHUNKS):
        dz_copy(c).wait()
        dh_copy(c).wait()


def table_kernel(dz_hbm, x_hbm, dh_hbm, dw_ref, loss_ref, out_hbm, dh_out, dw_out, loss_out,
                 dz_v, x_v, o_v, dh_v, x_sem, dz_sem, out_sem, dh_sem):
    n_blk = out_hbm.shape[0] // TT
    half = out_hbm.shape[1] // 2
    cuts = (slice(0, half), slice(half, 2 * half))

    def dz_copy(i):
        cols = pl.ds(pl.multiple_of(i * TT, TT), TT)
        return pltpu.make_async_copy(dz_hbm.at[:, cols], dz_v.at[:, cols], dz_sem.at[i])

    def out_copy(i, k):
        slot = lax.rem(i, SLOTS)
        rows = pl.ds(pl.multiple_of(i * TT, TT), TT)
        return pltpu.make_async_copy(o_v.at[slot, :, cuts[k]], out_hbm.at[rows, cuts[k]], out_sem.at[slot, k])

    def x_copy(k):
        return pltpu.make_async_copy(x_hbm.at[:, cuts[k]], x_v.at[:, cuts[k]], x_sem.at[k])

    dz_copy(0).start()
    x_copy(0).start()
    x_copy(1).start()

    @pl.loop(1, n_blk)
    def _(i):
        dz_copy(i).start()

    dh_in = pltpu.make_async_copy(dh_hbm, dh_v, dh_sem.at[0])
    dh_put = pltpu.make_async_copy(dh_v, dh_out, dh_sem.at[1])
    dh_in.start()
    dw_out[...] = dw_ref[...]
    loss_out[...] = loss_ref[...]
    x_copy(0).wait()
    x_copy(1).wait()
    @pl.loop(0, n_blk)
    def _(i):
        dz_copy(i).wait()

        @pl.when(i >= SLOTS)
        def _():
            out_copy(i - SLOTS, 0).wait()
            out_copy(i - SLOTS, 1).wait()

        cols = pl.ds(pl.multiple_of(i * TT, TT), TT)
        for k in range(2):
            o_v[lax.rem(i, SLOTS), :, cuts[k]] = lax.dot_general(
                dz_v[:, cols], x_v[:, cuts[k]], TN, preferred_element_type=F32)
            out_copy(i, k).start()

        @pl.when(i == 1)
        def _():
            dh_in.wait()
            dh_put.start()

    for i in range(n_blk - SLOTS, n_blk):
        out_copy(i, 0).wait()
        out_copy(i, 1).wait()
    dh_put.wait()


def solution(mesh):
    n_dev = mesh.shape['tp']

    def local_step(hidden, norm_gain, emb_block, teacher_ids, teacher_q):
        tokens, dim = hidden.shape
        vocab = emb_block.shape[0]
        rows_c = tokens // CHUNKS
        half = rows_c // 2
        kt = teacher_ids.shape[1]
        any_spec = pl.BlockSpec(memory_space=pl.ANY)
        vmem_spec = pl.BlockSpec(memory_space=pltpu.VMEM)
        vm = pltpu.VMEM
        dma = pltpu.SemaphoreType.DMA
        dh, dw, loss, dz, x_in = pl.pallas_call(
            lambda *refs: fused_kernel(n_dev, *refs),
            out_shape=(
                jax.ShapeDtypeStruct((tokens, dim), BF16),
                jax.ShapeDtypeStruct((dim,), F32),
                jax.ShapeDtypeStruct((1, 128), F32),
                jax.ShapeDtypeStruct((tokens, vocab), BF16),
                jax.ShapeDtypeStruct((tokens, dim), BF16),
            ),
            in_specs=[any_spec, vmem_spec, any_spec, any_spec, any_spec],
            out_specs=(any_spec, vmem_spec, vmem_spec, any_spec, any_spec),
            scratch_shapes=[
                vm((tokens, dim), BF16),
                vm((tokens, dim), BF16),
                vm((vocab, dim), BF16),
                vm((tokens, kt), jnp.int32),
                vm((tokens, kt), F32),
                vm((tokens, vocab), F32),
                vm((tokens, 128), F32),
                vm((tokens, 128), F32),
                vm((tokens, 128), F32),
                vm((tokens, 128), F32),
                vm((vocab // 128 * rows_c, 128), F32),
                vm((tokens, vocab), BF16),
                vm((tokens, dim), F32),
                vm((tokens, dim), BF16),
                vm((tokens, dim), F32),
                vm((CHUNKS, half, dim), F32),
                vm((CHUNKS, 2, half // 4, dim), F32),
                vm((CHUNKS, 2, half // 8, dim), F32),
                vm((HALVES, 1, 2 * tokens // HALVES), F32),
                vm((HALVES, n_dev, 1, 2 * tokens // HALVES), F32),
                vm((1, dim + 128), F32),
                vm((n_dev, 1, dim + 128), F32),
                vm((8, dim), F32),
                vm((16, 128), F32),
                dma((vocab // VT,)),
                dma((4,)),
                dma((1 + 2 * CHUNKS,)),
                dma((HALVES, n_dev - 1)),
                dma((HALVES, n_dev - 1)),
                dma((n_dev - 1,)),
                dma((n_dev - 1,)),
                dma((CHUNKS, 2, 10)),
                dma((CHUNKS, 2, 10)),
            ],
            compiler_params=pltpu.CompilerParams(
                collective_id=0, has_side_effects=True, vmem_limit_bytes=67_043_328),
            name='fused_head',
        )(hidden, norm_gain, emb_block, teacher_ids, teacher_q)
        grad_block, dh, dw, loss = pl.pallas_call(
            table_kernel,
            in_specs=[any_spec, any_spec, any_spec, vmem_spec, vmem_spec],
            out_specs=(any_spec, any_spec, vmem_spec, vmem_spec),
            out_shape=(
                jax.ShapeDtypeStruct((vocab, dim), F32),
                jax.ShapeDtypeStruct((tokens, dim), BF16),
                jax.ShapeDtypeStruct((dim,), F32),
                jax.ShapeDtypeStruct((1, 128), F32),
            ),
            scratch_shapes=[
                vm((tokens, vocab), BF16),
                vm((tokens, dim), BF16),
                vm((SLOTS, TT, dim), F32),
                vm((tokens, dim), BF16),
                dma((2,)),
                dma((vocab // TT,)),
                dma((SLOTS, 2)),
                dma((2,)),
            ],
            compiler_params=pltpu.CompilerParams(vmem_limit_bytes=67_043_328),
            name='table_grad',
        )(dz, x_in, dh, dw, loss)
        return (loss[0, 0:1], dh, dw, grad_block)

    return jax.shard_map(local_step, mesh=mesh, in_specs=(P('dp', None), P(None), P('tp', None), P('dp', None), P('dp', None)), out_specs=(P('dp'), P('dp', None), P('dp'), P(('dp', 'tp'), None)), check_vma=False)
```

```python
import jax
import jax.numpy as jnp
from jax import lax
from jax.experimental import pallas as pl
from jax.experimental.pallas import tpu as pltpu
from jax.sharding import PartitionSpec as P

MESH = pl.DeviceIdType.MESH
F32 = jnp.float32
BF16 = jnp.bfloat16
NT = (((1,), (1,)), ((), ()))
TN = (((0,), (0,)), ((), ()))
CHUNKS = 4
HALVES = 2
VT = 512
SLOTS = 3
TT = 512
TOK = 32


def fused_kernel(n_dev, h_hbm, w_ref, e_hbm, ids_hbm, q_hbm,
                 dh_hbm, dw_ref, loss_ref, dz_hbm, x_hbm,
                 h_v, x_v, e_v, ids_v, q_v, z_v, mx_v, sm_v, lz_v, sn_v, qs_v, dz_v, dx_v, dh_v, g_v,
                 r0_v, r1_v, r2_v, st_send, st_recv, fin_send, fin_recv, dwacc_v, qz_v,
                 e_sem, in_sem, out_sem, st_ss, st_rs, fin_ss, fin_rs, ss, rs):
    tokens, dim = h_v.shape
    vocab = e_v.shape[0]
    rows_c = tokens // CHUNKS
    groups = vocab // 128
    half = rows_c // 2
    n_blk = vocab // VT
    me = lax.axis_index('tp')
    dp = lax.axis_index('dp')
    core = me % 2
    xc = (me // 2) % 2
    yc = me // 4
    sib = me + 1 - 2 * core
    xn = me + 2 - 4 * xc
    yn = me + 4 - 8 * yc
    base = me * vocab
    inv_tokens = 1.0 / tokens

    def al(value, mult):
        return pl.multiple_of(value, mult)

    part = tokens // HALVES

    def h_copy(h):
        rows = slice(h * part, (h + 1) * part)
        return pltpu.make_async_copy(h_hbm.at[rows], h_v.at[rows], in_sem.at[3 * h])

    ids_copy = pltpu.make_async_copy(ids_hbm, ids_v, in_sem.at[1])
    q_copy = pltpu.make_async_copy(q_hbm, q_v, in_sem.at[2])
    q_copy.start()
    h_copy(0).start()

    def e_copy(i):
        rows = pl.ds(al(i * VT, VT), VT)
        return pltpu.make_async_copy(e_hbm.at[rows], e_v.at[rows], e_sem.at[i])

    @pl.loop(0, n_blk)
    def _(i):
        e_copy(i).start()

    h_copy(1).start()
    ids_copy.start()

    barrier = pltpu.get_barrier_semaphore()
    for i in range(1, n_dev):
        pl.semaphore_signal(barrier, inc=1, device_id=(dp, (me + i) % n_dev), device_id_type=MESH)

    q_copy.wait()

    @pl.loop(0, tokens // 64)
    def _(i):
        rows = pl.ds(al(i * 64, 64), 64)
        sn_v[rows, :] = jnp.broadcast_to(jnp.sum(q_v[rows, :], axis=1, keepdims=True), (64, 128))

    gain = w_ref[...].reshape(1, dim) + 1.0

    def norm(h):
        h_copy(h).wait()

        @pl.loop(0, part // 64)
        def _(i):
            rows = pl.ds(al(h * part + i * 64, 64), 64)
            acc = jnp.zeros((64, 128), F32)
            for k in range(dim // 128):
                hf = h_v[rows, 128 * k:128 * (k + 1)].astype(F32)
                acc = acc + hf * hf
            inv = lax.rsqrt(jnp.sum(acc, axis=1, keepdims=True) * (1.0 / dim) + 1e-6)
            inv = jnp.broadcast_to(inv, (64, 128))
            for k in range(dim // 128):
                hf = h_v[rows, 128 * k:128 * (k + 1)].astype(F32)
                x_v[rows, 128 * k:128 * (k + 1)] = (hf * inv * gain[:, 128 * k:128 * (k + 1)]).astype(BF16)

    mx_v[...] = jnp.full(mx_v.shape, -jnp.inf, F32)
    sm_v[...] = jnp.zeros(sm_v.shape, F32)

    def logits(h, first, last):
        rows = slice(h * part, (h + 1) * part)

        @pl.loop(first, last)
        def _(i):
            if h == 0:
                e_copy(i).wait()
            zb = lax.dot_general(x_v[rows, :], e_v[pl.ds(al(i * VT, VT), VT), :], NT, preferred_element_type=F32)
            z_v[rows, pl.ds(al(i * VT, VT), VT)] = zb
            old = mx_v[rows, :]
            new = old
            for k in range(VT // 128):
                new = jnp.maximum(new, zb[:, 128 * k:128 * (k + 1)])
            total = sm_v[rows, :] * jnp.exp(old - new)
            for k in range(VT // 128):
                total = total + jnp.exp(zb[:, 128 * k:128 * (k + 1)] - new)
            mx_v[rows, :] = new
            sm_v[rows, :] = total

    def gather_copies(src, dst, s_sem, r_sem):
        out = []
        for i in range(1, n_dev):
            out.append(pltpu.make_async_remote_copy(
                src_ref=src, dst_ref=dst.at[me], send_sem=s_sem.at[i - 1], recv_sem=r_sem.at[i - 1],
                device_id=(dp, (me + i) % n_dev), device_id_type=MESH))
        return out

    st_copies = [gather_copies(st_send.at[h], st_recv.at[h], st_ss.at[h], st_rs.at[h]) for h in range(HALVES)]

    def send_stats(h):
        for b in range(part // 128):
            span = slice(h * part + 128 * b, h * part + 128 * (b + 1))
            peaks = mx_v[span, :].T
            peak = jnp.max(peaks, axis=0, keepdims=True)
            st_send[h, :, 128 * b:128 * (b + 1)] = peak
            st_send[h, :, part + 128 * b:part + 128 * (b + 1)] = jnp.sum(
                sm_v[span, :].T * jnp.exp(peaks - peak), axis=0, keepdims=True)
        st_recv[h, me] = st_send[h]
        if h == 0:
            pl.semaphore_wait(barrier, n_dev - 1)
        for copy in st_copies[h]:
            copy.start()

    def take_stats(h):
        for copy in st_copies[h]:
            copy.wait_recv()
        peak = st_recv[h, 0][:, 0:part]
        for d in range(1, n_dev):
            peak = jnp.maximum(peak, st_recv[h, d][:, 0:part])
        total = jnp.zeros((1, part), F32)
        for d in range(n_dev):
            total = total + st_recv[h, d][:, part:2 * part] * jnp.exp(st_recv[h, d][:, 0:part] - peak)
        log_z = peak + jnp.log(total)
        for b in range(part // 128):
            lz_v[h * part + 128 * b:h * part + 128 * (b + 1), :] = jnp.broadcast_to(
                log_z[:, 128 * b:128 * (b + 1)], (128, 128)).T

    iota_hi = lax.broadcasted_iota(jnp.int32, (groups, 256), 0)
    iota_lo = lax.broadcasted_iota(jnp.int32, (128, 256), 0)

    def build_q(c, p):
        @pl.loop(p * rows_c // TOK // 2, (p + 1) * rows_c // TOK // 2)
        def _(t):
            for u in range(TOK):
                local = t * TOK + u
                row = pl.ds(c * rows_c + local, 1)
                ids = ids_v[row, :] - base
                qv = q_v[row, :]
                q_a = qv.astype(BF16).astype(F32)
                rest = qv - q_a
                q_b = rest.astype(BF16).astype(F32)
                q_c = rest - q_b
                hot_hi = lax.shift_right_arithmetic(ids, 7) == iota_hi
                hot_lo = jnp.where((ids & 127) == iota_lo, 1.0, 0.0).astype(BF16)
                parts = [jnp.where(hot_hi, part, 0.0).astype(BF16) for part in (q_a, q_b, q_c)]
                res = lax.dot_general(jnp.concatenate(parts, axis=0), hot_lo, NT, preferred_element_type=F32)
                dense = res[0:groups] + res[groups:2 * groups] + res[2 * groups:3 * groups]
                qs_v[pl.ds(local, groups, stride=rows_c), :] = dense

    def make_dz(c):
        @pl.loop(0, rows_c // 16)
        def _(i):
            off = al(i * 16, 16)
            rows = pl.ds(al(c * rows_c + off, 16), 16)
            lz = lz_v[rows, :]
            sn = sn_v[rows, :]
            acc = jnp.zeros((16, 128), F32)
            for k in range(groups):
                zz = z_v[rows, 128 * k:128 * (k + 1)]
                qq = qs_v[pl.ds(al(k * rows_c + off, 16), 16), :]
                acc = acc + qq * zz
                d = (jnp.exp(zz - lz) * sn - qq) * inv_tokens
                dz_v[rows, 128 * k:128 * (k + 1)] = d.astype(BF16)
            qz_v[...] = qz_v[...] + acc

    def make_dx(c, p):
        rows = slice(c * rows_c, (c + 1) * rows_c)

        @pl.loop(p * dim // 256 // 2, (p + 1) * dim // 256 // 2)
        def _(j):
            cols = pl.ds(al(j * 256, 256), 256)
            dx_v[rows, cols] = jnp.dot(dz_v[rows, :], e_v[:, cols], preferred_element_type=F32)

    def mdx2(c, p):
        rows = slice(c * rows_c, (c + 2) * rows_c)

        @pl.loop(p * dim // 256 // 2, (p + 1) * dim // 256 // 2)
        def _(j):
            cols = pl.ds(al(j * 256, 256), 256)
            dx_v[rows, cols] = jnp.dot(dz_v[rows, :], e_v[:, cols], preferred_element_type=F32)

    q8 = half // 8
    q4 = half // 4
    q2 = half // 2

    wide = dim // 2
    cut = (slice(0, wide), slice(wide, 2 * wide))

    def rcopy(src, dst, c, p, slot, dev):
        return pltpu.make_async_remote_copy(
            src_ref=src, dst_ref=dst, send_sem=ss.at[c, p, slot], recv_sem=rs.at[c, p, slot],
            device_id=(dp, dev), device_id_type=MESH)

    def mine(c):
        return c * rows_c + half * core

    sent = []

    def go(*copies):
        for copy in copies:
            copy.start()
            sent.append(copy)

    def dx_at(start, size, p):
        return dx_v.at[pl.ds(al(start, size), size), cut[p]]

    def g_at(start, size, p):
        return g_v.at[pl.ds(al(start, size), size), cut[p]]

    def s0(c, p):
        return rcopy(dx_at(c * rows_c + half * (1 - core), half, p), r0_v.at[c, :, cut[p]], c, p, 0, sib)

    def s1(c, p):
        a = rcopy(dx_at(mine(c) + q4 * (1 - xc), q4, p), r1_v.at[c, 0, :, cut[p]], c, p, 1, xn)
        b = rcopy(dx_at(mine(c) + q2 + q4 * (1 - yc), q4, p), r1_v.at[c, 1, :, cut[p]], c, p, 2, yn)
        return a, b

    def s2(c, p):
        a = rcopy(dx_at(mine(c) + q4 * xc + q8 * (1 - yc), q8, p), r2_v.at[c, 0, :, cut[p]], c, p, 3, yn)
        b = rcopy(dx_at(mine(c) + q2 + q4 * yc + q8 * (1 - xc), q8, p), r2_v.at[c, 1, :, cut[p]], c, p, 4, xn)
        return a, b

    def s3(c, p):
        a = g_at(mine(c) + q4 * xc + q8 * yc, q8, p)
        b = g_at(mine(c) + q2 + q4 * yc + q8 * xc, q8, p)
        return rcopy(a, a, c, p, 5, yn), rcopy(b, b, c, p, 6, xn)

    def s4(c, p):
        a = g_at(mine(c) + q4 * xc, q4, p)
        b = g_at(mine(c) + q2 + q4 * yc, q4, p)
        return rcopy(a, a, c, p, 7, xn), rcopy(b, b, c, p, 8, yn)

    def s5(c, p):
        a = g_at(mine(c), half, p)
        return rcopy(a, a, c, p, 9, sib)

    def f0(c, p):
        go(s0(c, p))

    def f1(c, p):
        s0(c, p).wait_recv()

        @pl.loop(0, half // 8)
        def _(i):
            rows = pl.ds(al(mine(c) + 8 * i, 8), 8)
            dx_v[rows, cut[p]] = dx_v[rows, cut[p]] + r0_v[c, pl.ds(al(8 * i, 8), 8), cut[p]]
        go(*s1(c, p))

    def f2(c, p):
        for copy in s1(c, p):
            copy.wait_recv()
        for k, start in ((0, mine(c) + q4 * xc), (1, mine(c) + q2 + q4 * yc)):
            rows = pl.ds(al(start, q4), q4)
            dx_v[rows, cut[p]] = dx_v[rows, cut[p]] + r1_v[c, k, :, cut[p]]
        go(*s2(c, p))

    def norm_back(c, k, block, side):
        rows16 = pl.ds(al(block, 16), 16)
        rows = pl.ds(al(block + q8 * side, q8), q8)
        hb = h_v[rows16, :].astype(F32)
        hf = jnp.where(side == 0, hb[0:8, :], hb[8:16, :])
        grad = dx_v[rows, :] + r2_v[c, k]
        inv = lax.rsqrt(jnp.mean(hf * hf, axis=1, keepdims=True) + 1e-6)
        scaled = grad * gain
        mean = jnp.sum(scaled * hf, axis=1, keepdims=True) * (1.0 / dim)
        g_v[rows, :] = scaled * inv - hf * (inv * inv * inv * mean)
        dwacc_v[...] = dwacc_v[...] + grad * hf * inv

    def f3(c):
        for p in range(2):
            for copy in s2(c, p):
                copy.wait_recv()
        norm_back(c, 0, mine(c) + q4 * xc, yc)
        norm_back(c, 1, mine(c) + q2 + q4 * yc, xc)
        for p in range(2):
            go(*s3(c, p))

    def f4(c, p):
        for copy in s3(c, p):
            copy.wait_recv()
        go(*s4(c, p))

    def f5(c, p):
        for copy in s4(c, p):
            copy.wait_recv()
        go(s5(c, p))

    def rows_of(c):
        return slice(c * rows_c, (c + 1) * rows_c)

    def dh_copy(c):
        return pltpu.make_async_copy(dh_v.at[rows_of(c)], dh_hbm.at[rows_of(c)], out_sem.at[1 + c])

    def dz_copy(c):
        return pltpu.make_async_copy(dz_v.at[rows_of(c)], dz_hbm.at[rows_of(c)], out_sem.at[1 + CHUNKS + c])

    def f6(c):
        for p in range(2):
            s5(c, p).wait_recv()

        @pl.loop(0, rows_c // 16)
        def _(i):
            rows = pl.ds(al(c * rows_c + 16 * i, 16), 16)
            dh_v[rows, :] = g_v[rows, :].astype(BF16)
        dh_copy(c).start()

    dwacc_v[...] = jnp.zeros(dwacc_v.shape, F32)
    qz_v[...] = jnp.zeros(qz_v.shape, F32)

    def finish_dz(c):
        make_dz(c)
        dz_copy(c).start()

    quarter = n_blk // 4
    norm(0)
    logits(0, 0, n_blk)
    send_stats(0)
    norm(1)
    x_copy = pltpu.make_async_copy(x_v, x_hbm, out_sem.at[0])
    x_copy.start()
    ids_copy.wait()
    build_q(0, 0)
    build_q(0, 1)
    take_stats(0)
    finish_dz(0)
    build_q(1, 0)
    build_q(1, 1)
    finish_dz(1)
    mdx2(0, 0)
    f0(0, 0)
    f0(1, 0)
    mdx2(0, 1)
    f0(1, 1)
    f1(0, 0)
    f0(0, 1)
    logits(1, 0, quarter)
    f1(1, 0)
    logits(1, quarter, 2 * quarter)
    f1(1, 1)
    f1(0, 1)
    logits(1, 2 * quarter, 3 * quarter)
    f2(1, 0)
    logits(1, 3 * quarter, n_blk)
    send_stats(1)
    f2(1, 1)
    f2(0, 0)
    build_q(2, 0)
    f2(0, 1)
    build_q(2, 1)
    f3(1)
    take_stats(1)
    finish_dz(2)
    f3(0)
    make_dx(2, 1)
    f0(2, 1)
    f4(1, 0)
    f4(1, 1)
    make_dx(2, 0)
    f4(0, 1)
    f0(2, 0)
    build_q(3, 0)
    f1(2, 1)
    build_q(3, 1)
    finish_dz(3)
    f1(2, 0)
    f4(0, 0)
    make_dx(3, 1)
    f2(2, 1)
    f0(3, 1)
    make_dx(3, 0)
    f0(3, 0)
    f2(2, 0)
    f1(3, 1)
    f1(3, 0)
    f5(0, 1)
    f3(2)
    f2(3, 1)
    f5(0, 0)
    f5(1, 1)
    f2(3, 0)
    f4(2, 0)
    f5(1, 0)
    f3(3)
    f4(2, 1)
    fin_send[:, 0:dim] = jnp.sum(dwacc_v[...], axis=0, keepdims=True)
    fin_send[:, dim:dim + 128] = jnp.sum(qz_v[...], axis=0, keepdims=True)
    fin_recv[me] = fin_send[...]
    fin_copies = gather_copies(fin_send, fin_recv, fin_ss, fin_rs)
    for copy in fin_copies:
        copy.start()
    f4(3, 0)
    f4(3, 1)
    f6(0)
    f5(3, 0)
    f5(2, 1)
    f5(2, 0)
    f6(1)
    f5(3, 1)
    f6(2)

    for copy in fin_copies:
        copy.wait_recv()
    fin = fin_recv[0]
    for d in range(1, n_dev):
        fin = fin + fin_recv[d]
    dw_ref[...] = fin[:, 0:dim].reshape(dim)
    weighted = jnp.sum(lz_v[...] * sn_v[...], axis=0, keepdims=True)
    loss_ref[...] = (weighted - jnp.sum(fin[:, dim:dim + 128])) * inv_tokens
    f6(3)

    for copy in st_copies[0] + st_copies[1] + sent + fin_copies:
        copy.wait_send()
    x_copy.wait()
    for c in range(CHUNKS):
        dz_copy(c).wait()
        dh_copy(c).wait()


def table_kernel(dz_hbm, x_hbm, dh_hbm, dw_ref, loss_ref, out_hbm, dh_out, dw_out, loss_out,
                 dz_v, x_v, o_v, dh_v, x_sem, dz_sem, out_sem, dh_sem):
    n_blk = out_hbm.shape[0] // TT
    half = out_hbm.shape[1] // 2
    cuts = (slice(0, half), slice(half, 2 * half))

    def dz_copy(i):
        cols = pl.ds(pl.multiple_of(i * TT, TT), TT)
        return pltpu.make_async_copy(dz_hbm.at[:, cols], dz_v.at[:, cols], dz_sem.at[i])

    def out_copy(i, k):
        slot = lax.rem(i, SLOTS)
        rows = pl.ds(pl.multiple_of(i * TT, TT), TT)
        return pltpu.make_async_copy(o_v.at[slot, :, cuts[k]], out_hbm.at[rows, cuts[k]], out_sem.at[slot, k])

    def x_copy(k):
        return pltpu.make_async_copy(x_hbm.at[:, cuts[k]], x_v.at[:, cuts[k]], x_sem.at[k])

    dz_copy(0).start()
    x_copy(0).start()
    x_copy(1).start()

    @pl.loop(1, n_blk)
    def _(i):
        dz_copy(i).start()

    dh_in = pltpu.make_async_copy(dh_hbm, dh_v, dh_sem.at[0])
    dh_put = pltpu.make_async_copy(dh_v, dh_out, dh_sem.at[1])
    dh_in.start()
    dw_out[...] = dw_ref[...]
    loss_out[...] = loss_ref[...]
    x_copy(0).wait()
    x_copy(1).wait()
    @pl.loop(0, n_blk)
    def _(i):
        dz_copy(i).wait()

        @pl.when(i >= SLOTS)
        def _():
            out_copy(i - SLOTS, 0).wait()
            out_copy(i - SLOTS, 1).wait()

        cols = pl.ds(pl.multiple_of(i * TT, TT), TT)
        for k in range(2):
            o_v[lax.rem(i, SLOTS), :, cuts[k]] = lax.dot_general(
                dz_v[:, cols], x_v[:, cuts[k]], TN, preferred_element_type=F32)
            out_copy(i, k).start()

        @pl.when(i == 1)
        def _():
            dh_in.wait()
            dh_put.start()

    for i in range(n_blk - SLOTS, n_blk):
        out_copy(i, 0).wait()
        out_copy(i, 1).wait()
    dh_put.wait()


def solution(mesh):
    n_dev = mesh.shape['tp']

    def local_step(hidden, norm_gain, emb_block, teacher_ids, teacher_q):
        tokens, dim = hidden.shape
        vocab = emb_block.shape[0]
        rows_c = tokens // CHUNKS
        half = rows_c // 2
        kt = teacher_ids.shape[1]
        any_spec = pl.BlockSpec(memory_space=pl.ANY)
        vmem_spec = pl.BlockSpec(memory_space=pltpu.VMEM)
        vm = pltpu.VMEM
        dma = pltpu.SemaphoreType.DMA
        dh, dw, loss, dz, x_in = pl.pallas_call(
            lambda *refs: fused_kernel(n_dev, *refs),
            out_shape=(
                jax.ShapeDtypeStruct((tokens, dim), BF16),
                jax.ShapeDtypeStruct((dim,), F32),
                jax.ShapeDtypeStruct((1, 128), F32),
                jax.ShapeDtypeStruct((tokens, vocab), BF16),
                jax.ShapeDtypeStruct((tokens, dim), BF16),
            ),
            in_specs=[any_spec, vmem_spec, any_spec, any_spec, any_spec],
            out_specs=(any_spec, vmem_spec, vmem_spec, any_spec, any_spec),
            scratch_shapes=[
                vm((tokens, dim), BF16),
                vm((tokens, dim), BF16),
                vm((vocab, dim), BF16),
                vm((tokens, kt), jnp.int32),
                vm((tokens, kt), F32),
                vm((tokens, vocab), F32),
                vm((tokens, 128), F32),
                vm((tokens, 128), F32),
                vm((tokens, 128), F32),
                vm((tokens, 128), F32),
                vm((vocab // 128 * rows_c, 128), F32),
                vm((tokens, vocab), BF16),
                vm((tokens, dim), F32),
                vm((tokens, dim), BF16),
                vm((tokens, dim), F32),
                vm((CHUNKS, half, dim), F32),
                vm((CHUNKS, 2, half // 4, dim), F32),
                vm((CHUNKS, 2, half // 8, dim), F32),
                vm((HALVES, 1, 2 * tokens // HALVES), F32),
                vm((HALVES, n_dev, 1, 2 * tokens // HALVES), F32),
                vm((1, dim + 128), F32),
                vm((n_dev, 1, dim + 128), F32),
                vm((8, dim), F32),
                vm((16, 128), F32),
                dma((vocab // VT,)),
                dma((4,)),
                dma((1 + 2 * CHUNKS,)),
                dma((HALVES, n_dev - 1)),
                dma((HALVES, n_dev - 1)),
                dma((n_dev - 1,)),
                dma((n_dev - 1,)),
                dma((CHUNKS, 2, 10)),
                dma((CHUNKS, 2, 10)),
            ],
            compiler_params=pltpu.CompilerParams(
                collective_id=0, has_side_effects=True, vmem_limit_bytes=67_043_328),
            name='fused_head',
        )(hidden, norm_gain, emb_block, teacher_ids, teacher_q)
        grad_block, dh, dw, loss = pl.pallas_call(
            table_kernel,
            in_specs=[any_spec, any_spec, any_spec, vmem_spec, vmem_spec],
            out_specs=(any_spec, any_spec, vmem_spec, vmem_spec),
            out_shape=(
                jax.ShapeDtypeStruct((vocab, dim), F32),
                jax.ShapeDtypeStruct((tokens, dim), BF16),
                jax.ShapeDtypeStruct((dim,), F32),
                jax.ShapeDtypeStruct((1, 128), F32),
            ),
            scratch_shapes=[
                vm((tokens, vocab), BF16),
                vm((tokens, dim), BF16),
                vm((SLOTS, TT, dim), F32),
                vm((tokens, dim), BF16),
                dma((2,)),
                dma((vocab // TT,)),
                dma((SLOTS, 2)),
                dma((2,)),
            ],
            compiler_params=pltpu.CompilerParams(vmem_limit_bytes=67_043_328),
            name='table_grad',
        )(dz, x_in, dh, dw, loss)
        return (loss[0, 0:1], dh, dw, grad_block)

    return jax.shard_map(local_step, mesh=mesh, in_specs=(P('dp', None), P(None), P('tp', None), P('dp', None), P('dp', None)), out_specs=(P('dp'), P('dp', None), P('dp'), P(('dp', 'tp'), None)), check_vma=False)
```

```python
import jax
import jax.numpy as jnp
from jax import lax
from jax.experimental import pallas as pl
from jax.experimental.pallas import tpu as pltpu
from jax.sharding import PartitionSpec as P

MESH = pl.DeviceIdType.MESH
F32 = jnp.float32
BF16 = jnp.bfloat16
NT = (((1,), (1,)), ((), ()))
TN = (((0,), (0,)), ((), ()))
CHUNKS = 4
HALVES = 2
VT = 512
SLOTS = 3
TT = 512
TOK = 32


def fused_kernel(n_dev, h_hbm, w_ref, e_hbm, ids_hbm, q_hbm,
                 dh_hbm, dw_ref, loss_ref, dz_hbm, x_hbm,
                 h_v, x_v, e_v, ids_v, q_v, z_v, mx_v, sm_v, lz_v, sn_v, qs_v, dz_v, dx_v, dh_v, g_v,
                 r0_v, r1_v, r2_v, st_send, st_recv, fin_send, fin_recv, dwacc_v, qz_v,
                 e_sem, in_sem, out_sem, st_ss, st_rs, fin_ss, fin_rs, ss, rs):
    tokens, dim = h_v.shape
    vocab = e_v.shape[0]
    rows_c = tokens // CHUNKS
    groups = vocab // 128
    half = rows_c // 2
    n_blk = vocab // VT
    me = lax.axis_index('tp')
    dp = lax.axis_index('dp')
    core = me % 2
    xc = (me // 2) % 2
    yc = me // 4
    sib = me + 1 - 2 * core
    xn = me + 2 - 4 * xc
    yn = me + 4 - 8 * yc
    base = me * vocab
    inv_tokens = 1.0 / tokens

    def al(value, mult):
        return pl.multiple_of(value, mult)

    part = tokens // HALVES

    def h_copy(h):
        rows = slice(h * part, (h + 1) * part)
        return pltpu.make_async_copy(h_hbm.at[rows], h_v.at[rows], in_sem.at[3 * h])

    ids_copy = pltpu.make_async_copy(ids_hbm, ids_v, in_sem.at[1])
    q_copy = pltpu.make_async_copy(q_hbm, q_v, in_sem.at[2])
    q_copy.start()
    h_copy(0).start()

    def e_copy(i):
        rows = pl.ds(al(i * VT, VT), VT)
        return pltpu.make_async_copy(e_hbm.at[rows], e_v.at[rows], e_sem.at[i])

    @pl.loop(0, n_blk)
    def _(i):
        e_copy(i).start()

    h_copy(1).start()
    ids_copy.start()

    barrier = pltpu.get_barrier_semaphore()
    for i in range(1, n_dev):
        pl.semaphore_signal(barrier, inc=1, device_id=(dp, (me + i) % n_dev), device_id_type=MESH)

    q_copy.wait()

    @pl.loop(0, tokens // 64)
    def _(i):
        rows = pl.ds(al(i * 64, 64), 64)
        sn_v[rows, :] = jnp.broadcast_to(jnp.sum(q_v[rows, :], axis=1, keepdims=True), (64, 128))

    gain = w_ref[...].reshape(1, dim) + 1.0

    def norm(h):
        h_copy(h).wait()

        @pl.loop(0, part // 64)
        def _(i):
            rows = pl.ds(al(h * part + i * 64, 64), 64)
            acc = jnp.zeros((64, 128), F32)
            for k in range(dim // 128):
                hf = h_v[rows, 128 * k:128 * (k + 1)].astype(F32)
                acc = acc + hf * hf
            inv = lax.rsqrt(jnp.sum(acc, axis=1, keepdims=True) * (1.0 / dim) + 1e-6)
            inv = jnp.broadcast_to(inv, (64, 128))
            for k in range(dim // 128):
                hf = h_v[rows, 128 * k:128 * (k + 1)].astype(F32)
                x_v[rows, 128 * k:128 * (k + 1)] = (hf * inv * gain[:, 128 * k:128 * (k + 1)]).astype(BF16)

    mx_v[...] = jnp.full(mx_v.shape, -jnp.inf, F32)
    sm_v[...] = jnp.zeros(sm_v.shape, F32)

    def logits(h, first, last):
        rows = slice(h * part, (h + 1) * part)

        @pl.loop(first, last)
        def _(i):
            if h == 0:
                e_copy(i).wait()
            zb = lax.dot_general(x_v[rows, :], e_v[pl.ds(al(i * VT, VT), VT), :], NT, preferred_element_type=F32)
            z_v[rows, pl.ds(al(i * VT, VT), VT)] = zb
            old = mx_v[rows, :]
            new = old
            for k in range(VT // 128):
                new = jnp.maximum(new, zb[:, 128 * k:128 * (k + 1)])
            total = sm_v[rows, :] * jnp.exp(old - new)
            for k in range(VT // 128):
                total = total + jnp.exp(zb[:, 128 * k:128 * (k + 1)] - new)
            mx_v[rows, :] = new
            sm_v[rows, :] = total

    def gather_copies(src, dst, s_sem, r_sem):
        out = []
        for i in range(1, n_dev):
            out.append(pltpu.make_async_remote_copy(
                src_ref=src, dst_ref=dst.at[me], send_sem=s_sem.at[i - 1], recv_sem=r_sem.at[i - 1],
                device_id=(dp, (me + i) % n_dev), device_id_type=MESH))
        return out

    st_copies = [gather_copies(st_send.at[h], st_recv.at[h], st_ss.at[h], st_rs.at[h]) for h in range(HALVES)]

    def send_stats(h):
        for b in range(part // 128):
            span = slice(h * part + 128 * b, h * part + 128 * (b + 1))
            peaks = mx_v[span, :].T
            peak = jnp.max(peaks, axis=0, keepdims=True)
            st_send[h, :, 128 * b:128 * (b + 1)] = peak
            st_send[h, :, part + 128 * b:part + 128 * (b + 1)] = jnp.sum(
                sm_v[span, :].T * jnp.exp(peaks - peak), axis=0, keepdims=True)
        st_recv[h, me] = st_send[h]
        if h == 0:
            pl.semaphore_wait(barrier, n_dev - 1)
        for copy in st_copies[h]:
            copy.start()

    def take_stats(h):
        for copy in st_copies[h]:
            copy.wait_recv()
        peak = st_recv[h, 0][:, 0:part]
        for d in range(1, n_dev):
            peak = jnp.maximum(peak, st_recv[h, d][:, 0:part])
        total = jnp.zeros((1, part), F32)
        for d in range(n_dev):
            total = total + st_recv[h, d][:, part:2 * part] * jnp.exp(st_recv[h, d][:, 0:part] - peak)
        log_z = peak + jnp.log(total)
        for b in range(part // 128):
            lz_v[h * part + 128 * b:h * part + 128 * (b + 1), :] = jnp.broadcast_to(
                log_z[:, 128 * b:128 * (b + 1)], (128, 128)).T

    iota_hi = lax.broadcasted_iota(jnp.int32, (groups, 256), 0)
    iota_lo = lax.broadcasted_iota(jnp.int32, (128, 256), 0)

    def build_q(c, p):
        @pl.loop(p * rows_c // TOK // 2, (p + 1) * rows_c // TOK // 2)
        def _(t):
            for u in range(TOK):
                local = t * TOK + u
                row = pl.ds(c * rows_c + local, 1)
                ids = ids_v[row, :] - base
                qv = q_v[row, :]
                q_a = qv.astype(BF16).astype(F32)
                rest = qv - q_a
                q_b = rest.astype(BF16).astype(F32)
                q_c = rest - q_b
                hot_hi = lax.shift_right_arithmetic(ids, 7) == iota_hi
                hot_lo = jnp.where((ids & 127) == iota_lo, 1.0, 0.0).astype(BF16)
                parts = [jnp.where(hot_hi, part, 0.0).astype(BF16) for part in (q_a, q_b, q_c)]
                res = lax.dot_general(jnp.concatenate(parts, axis=0), hot_lo, NT, preferred_element_type=F32)
                dense = res[0:groups] + res[groups:2 * groups] + res[2 * groups:3 * groups]
                qs_v[pl.ds(local, groups, stride=rows_c), :] = dense

    def make_dz(c):
        @pl.loop(0, rows_c // 16)
        def _(i):
            off = al(i * 16, 16)
            rows = pl.ds(al(c * rows_c + off, 16), 16)
            lz = lz_v[rows, :]
            sn = sn_v[rows, :]
            acc = jnp.zeros((16, 128), F32)
            for k in range(groups):
                zz = z_v[rows, 128 * k:128 * (k + 1)]
                qq = qs_v[pl.ds(al(k * rows_c + off, 16), 16), :]
                acc = acc + qq * zz
                d = (jnp.exp(zz - lz) * sn - qq) * inv_tokens
                dz_v[rows, 128 * k:128 * (k + 1)] = d.astype(BF16)
            qz_v[...] = qz_v[...] + acc

    def make_dx(c, p):
        rows = slice(c * rows_c, (c + 1) * rows_c)

        @pl.loop(p * dim // 256 // 2, (p + 1) * dim // 256 // 2)
        def _(j):
            cols = pl.ds(al(j * 256, 256), 256)
            dx_v[rows, cols] = jnp.dot(dz_v[rows, :], e_v[:, cols], preferred_element_type=F32)

    def mdx2(c, p):
        rows = slice(c * rows_c, (c + 2) * rows_c)

        @pl.loop(p * dim // 256 // 2, (p + 1) * dim // 256 // 2)
        def _(j):
            cols = pl.ds(al(j * 256, 256), 256)
            dx_v[rows, cols] = jnp.dot(dz_v[rows, :], e_v[:, cols], preferred_element_type=F32)

    q8 = half // 8
    q4 = half // 4
    q2 = half // 2

    wide = dim // 2
    cut = (slice(0, wide), slice(wide, 2 * wide))

    def rcopy(src, dst, c, p, slot, dev):
        return pltpu.make_async_remote_copy(
            src_ref=src, dst_ref=dst, send_sem=ss.at[c, p, slot], recv_sem=rs.at[c, p, slot],
            device_id=(dp, dev), device_id_type=MESH)

    def mine(c):
        return c * rows_c + half * core

    sent = []

    def go(*copies):
        for copy in copies:
            copy.start()
            sent.append(copy)

    def dx_at(start, size, p):
        return dx_v.at[pl.ds(al(start, size), size), cut[p]]

    def g_at(start, size, p):
        return g_v.at[pl.ds(al(start, size), size), cut[p]]

    def s0(c, p):
        return rcopy(dx_at(c * rows_c + half * (1 - core), half, p), r0_v.at[c, :, cut[p]], c, p, 0, sib)

    def s1(c, p):
        a = rcopy(dx_at(mine(c) + q4 * (1 - xc), q4, p), r1_v.at[c, 0, :, cut[p]], c, p, 1, xn)
        b = rcopy(dx_at(mine(c) + q2 + q4 * (1 - yc), q4, p), r1_v.at[c, 1, :, cut[p]], c, p, 2, yn)
        return a, b

    def s2(c, p):
        a = rcopy(dx_at(mine(c) + q4 * xc + q8 * (1 - yc), q8, p), r2_v.at[c, 0, :, cut[p]], c, p, 3, yn)
        b = rcopy(dx_at(mine(c) + q2 + q4 * yc + q8 * (1 - xc), q8, p), r2_v.at[c, 1, :, cut[p]], c, p, 4, xn)
        return a, b

    def s3(c, p):
        a = g_at(mine(c) + q4 * xc + q8 * yc, q8, p)
        b = g_at(mine(c) + q2 + q4 * yc + q8 * xc, q8, p)
        return rcopy(a, a, c, p, 5, yn), rcopy(b, b, c, p, 6, xn)

    def s4(c, p):
        a = g_at(mine(c) + q4 * xc, q4, p)
        b = g_at(mine(c) + q2 + q4 * yc, q4, p)
        return rcopy(a, a, c, p, 7, xn), rcopy(b, b, c, p, 8, yn)

    def s5(c, p):
        a = g_at(mine(c), half, p)
        return rcopy(a, a, c, p, 9, sib)

    def f0(c, p):
        go(s0(c, p))

    def f1(c, p):
        s0(c, p).wait_recv()

        @pl.loop(0, half // 8)
        def _(i):
            rows = pl.ds(al(mine(c) + 8 * i, 8), 8)
            dx_v[rows, cut[p]] = dx_v[rows, cut[p]] + r0_v[c, pl.ds(al(8 * i, 8), 8), cut[p]]
        go(*s1(c, p))

    def f2(c, p):
        for copy in s1(c, p):
            copy.wait_recv()
        for k, start in ((0, mine(c) + q4 * xc), (1, mine(c) + q2 + q4 * yc)):
            rows = pl.ds(al(start, q4), q4)
            dx_v[rows, cut[p]] = dx_v[rows, cut[p]] + r1_v[c, k, :, cut[p]]
        go(*s2(c, p))

    def norm_back(c, k, block, side):
        rows16 = pl.ds(al(block, 16), 16)
        rows = pl.ds(al(block + q8 * side, q8), q8)
        hb = h_v[rows16, :].astype(F32)
        hf = jnp.where(side == 0, hb[0:8, :], hb[8:16, :])
        grad = dx_v[rows, :] + r2_v[c, k]
        inv = lax.rsqrt(jnp.mean(hf * hf, axis=1, keepdims=True) + 1e-6)
        scaled = grad * gain
        mean = jnp.sum(scaled * hf, axis=1, keepdims=True) * (1.0 / dim)
        g_v[rows, :] = scaled * inv - hf * (inv * inv * inv * mean)
        dwacc_v[...] = dwacc_v[...] + grad * hf * inv

    def f3(c):
        for p in range(2):
            for copy in s2(c, p):
                copy.wait_recv()
        norm_back(c, 0, mine(c) + q4 * xc, yc)
        norm_back(c, 1, mine(c) + q2 + q4 * yc, xc)
        for p in range(2):
            go(*s3(c, p))

    def f4(c, p):
        for copy in s3(c, p):
            copy.wait_recv()
        go(*s4(c, p))

    def f5(c, p):
        for copy in s4(c, p):
            copy.wait_recv()
        go(s5(c, p))

    def rows_of(c):
        return slice(c * rows_c, (c + 1) * rows_c)

    def dh_copy(c):
        return pltpu.make_async_copy(dh_v.at[rows_of(c)], dh_hbm.at[rows_of(c)], out_sem.at[1 + c])

    def dz_copy(c):
        return pltpu.make_async_copy(dz_v.at[rows_of(c)], dz_hbm.at[rows_of(c)], out_sem.at[1 + CHUNKS + c])

    def f6(c):
        for p in range(2):
            s5(c, p).wait_recv()

        @pl.loop(0, rows_c // 16)
        def _(i):
            rows = pl.ds(al(c * rows_c + 16 * i, 16), 16)
            dh_v[rows, :] = g_v[rows, :].astype(BF16)
        dh_copy(c).start()

    def last_copy(p):
        rows = rows_of(CHUNKS - 1)
        return pltpu.make_async_copy(
            dh_v.at[rows, cut[p]], dh_hbm.at[rows, cut[p]], out_sem.at[CHUNKS if p == 0 else 1 + 2 * CHUNKS])

    def f6_last():
        c = CHUNKS - 1
        for p in range(2):
            s5(c, p).wait_recv()

            @pl.loop(0, rows_c // 16)
            def _(i):
                rows = pl.ds(al(c * rows_c + 16 * i, 16), 16)
                dh_v[rows, cut[p]] = g_v[rows, cut[p]].astype(BF16)
            last_copy(p).start()

    dwacc_v[...] = jnp.zeros(dwacc_v.shape, F32)
    qz_v[...] = jnp.zeros(qz_v.shape, F32)

    def finish_dz(c):
        make_dz(c)
        dz_copy(c).start()

    quarter = n_blk // 4
    norm(0)
    logits(0, 0, n_blk)
    send_stats(0)
    norm(1)
    x_copy = pltpu.make_async_copy(x_v, x_hbm, out_sem.at[0])
    x_copy.start()
    ids_copy.wait()
    build_q(0, 0)
    build_q(0, 1)
    take_stats(0)
    finish_dz(0)
    build_q(1, 0)
    build_q(1, 1)
    finish_dz(1)
    mdx2(0, 0)
    f0(0, 0)
    f0(1, 0)
    mdx2(0, 1)
    f0(1, 1)
    f1(0, 0)
    f0(0, 1)
    logits(1, 0, quarter)
    f1(1, 0)
    logits(1, quarter, 2 * quarter)
    f1(1, 1)
    f1(0, 1)
    logits(1, 2 * quarter, 3 * quarter)
    f2(1, 0)
    logits(1, 3 * quarter, n_blk)
    send_stats(1)
    f2(1, 1)
    f2(0, 0)
    build_q(2, 0)
    f2(0, 1)
    build_q(2, 1)
    f3(1)
    take_stats(1)
    finish_dz(2)
    f3(0)
    make_dx(2, 1)
    f0(2, 1)
    f4(1, 0)
    f4(1, 1)
    make_dx(2, 0)
    f4(0, 1)
    f0(2, 0)
    build_q(3, 0)
    f1(2, 1)
    build_q(3, 1)
    finish_dz(3)
    f1(2, 0)
    f4(0, 0)
    make_dx(3, 1)
    f2(2, 1)
    f0(3, 1)
    make_dx(3, 0)
    f0(3, 0)
    f2(2, 0)
    f1(3, 1)
    f1(3, 0)
    f5(0, 1)
    f3(2)
    f2(3, 1)
    f5(0, 0)
    f5(1, 1)
    f2(3, 0)
    f4(2, 0)
    f5(1, 0)
    f3(3)
    f4(2, 1)
    fin_send[:, 0:dim] = jnp.sum(dwacc_v[...], axis=0, keepdims=True)
    fin_send[:, dim:dim + 128] = jnp.sum(qz_v[...], axis=0, keepdims=True)
    fin_recv[me] = fin_send[...]
    fin_copies = gather_copies(fin_send, fin_recv, fin_ss, fin_rs)
    for copy in fin_copies:
        copy.start()
    f4(3, 0)
    f4(3, 1)
    f6(0)
    f5(3, 0)
    f5(2, 1)
    f5(2, 0)
    f6(1)
    f5(3, 1)
    f6(2)

    for copy in fin_copies:
        copy.wait_recv()
    fin = fin_recv[0]
    for d in range(1, n_dev):
        fin = fin + fin_recv[d]
    dw_ref[...] = fin[:, 0:dim].reshape(dim)
    weighted = jnp.sum(lz_v[...] * sn_v[...], axis=0, keepdims=True)
    loss_ref[...] = (weighted - jnp.sum(fin[:, dim:dim + 128])) * inv_tokens
    f6_last()

    for copy in st_copies[0] + st_copies[1] + sent + fin_copies:
        copy.wait_send()
    x_copy.wait()
    for c in range(CHUNKS):
        dz_copy(c).wait()
        if c < CHUNKS - 1:
            dh_copy(c).wait()
    for p in range(2):
        last_copy(p).wait()


def table_kernel(dz_hbm, x_hbm, dh_hbm, dw_ref, loss_ref, out_hbm, dh_out, dw_out, loss_out,
                 dz_v, x_v, o_v, dh_v, x_sem, dz_sem, out_sem, dh_sem):
    n_blk = out_hbm.shape[0] // TT
    half = out_hbm.shape[1] // 2
    cuts = (slice(0, half), slice(half, 2 * half))

    def dz_copy(i):
        cols = pl.ds(pl.multiple_of(i * TT, TT), TT)
        return pltpu.make_async_copy(dz_hbm.at[:, cols], dz_v.at[:, cols], dz_sem.at[i])

    def out_copy(i, k):
        slot = lax.rem(i, SLOTS)
        rows = pl.ds(pl.multiple_of(i * TT, TT), TT)
        return pltpu.make_async_copy(o_v.at[slot, :, cuts[k]], out_hbm.at[rows, cuts[k]], out_sem.at[slot, k])

    def x_copy(k):
        return pltpu.make_async_copy(x_hbm.at[:, cuts[k]], x_v.at[:, cuts[k]], x_sem.at[k])

    dz_copy(0).start()
    x_copy(0).start()
    x_copy(1).start()

    @pl.loop(1, n_blk)
    def _(i):
        dz_copy(i).start()

    dh_in = pltpu.make_async_copy(dh_hbm, dh_v, dh_sem.at[0])
    dh_put = pltpu.make_async_copy(dh_v, dh_out, dh_sem.at[1])
    dh_in.start()
    dw_out[...] = dw_ref[...]
    loss_out[...] = loss_ref[...]
    x_copy(0).wait()
    x_copy(1).wait()
    @pl.loop(0, n_blk)
    def _(i):
        dz_copy(i).wait()

        @pl.when(i >= SLOTS)
        def _():
            out_copy(i - SLOTS, 0).wait()
            out_copy(i - SLOTS, 1).wait()

        cols = pl.ds(pl.multiple_of(i * TT, TT), TT)
        for k in range(2):
            o_v[lax.rem(i, SLOTS), :, cuts[k]] = lax.dot_general(
                dz_v[:, cols], x_v[:, cuts[k]], TN, preferred_element_type=F32)
            out_copy(i, k).start()

        @pl.when(i == 1)
        def _():
            dh_in.wait()
            dh_put.start()

    for i in range(n_blk - SLOTS, n_blk):
        out_copy(i, 0).wait()
        out_copy(i, 1).wait()
    dh_put.wait()


def solution(mesh):
    n_dev = mesh.shape['tp']

    def local_step(hidden, norm_gain, emb_block, teacher_ids, teacher_q):
        tokens, dim = hidden.shape
        vocab = emb_block.shape[0]
        rows_c = tokens // CHUNKS
        half = rows_c // 2
        kt = teacher_ids.shape[1]
        any_spec = pl.BlockSpec(memory_space=pl.ANY)
        vmem_spec = pl.BlockSpec(memory_space=pltpu.VMEM)
        vm = pltpu.VMEM
        dma = pltpu.SemaphoreType.DMA
        dh, dw, loss, dz, x_in = pl.pallas_call(
            lambda *refs: fused_kernel(n_dev, *refs),
            out_shape=(
                jax.ShapeDtypeStruct((tokens, dim), BF16),
                jax.ShapeDtypeStruct((dim,), F32),
                jax.ShapeDtypeStruct((1, 128), F32),
                jax.ShapeDtypeStruct((tokens, vocab), BF16),
                jax.ShapeDtypeStruct((tokens, dim), BF16),
            ),
            in_specs=[any_spec, vmem_spec, any_spec, any_spec, any_spec],
            out_specs=(any_spec, vmem_spec, vmem_spec, any_spec, any_spec),
            scratch_shapes=[
                vm((tokens, dim), BF16),
                vm((tokens, dim), BF16),
                vm((vocab, dim), BF16),
                vm((tokens, kt), jnp.int32),
                vm((tokens, kt), F32),
                vm((tokens, vocab), F32),
                vm((tokens, 128), F32),
                vm((tokens, 128), F32),
                vm((tokens, 128), F32),
                vm((tokens, 128), F32),
                vm((vocab // 128 * rows_c, 128), F32),
                vm((tokens, vocab), BF16),
                vm((tokens, dim), F32),
                vm((tokens, dim), BF16),
                vm((tokens, dim), F32),
                vm((CHUNKS, half, dim), F32),
                vm((CHUNKS, 2, half // 4, dim), F32),
                vm((CHUNKS, 2, half // 8, dim), F32),
                vm((HALVES, 1, 2 * tokens // HALVES), F32),
                vm((HALVES, n_dev, 1, 2 * tokens // HALVES), F32),
                vm((1, dim + 128), F32),
                vm((n_dev, 1, dim + 128), F32),
                vm((8, dim), F32),
                vm((16, 128), F32),
                dma((vocab // VT,)),
                dma((4,)),
                dma((2 + 2 * CHUNKS,)),
                dma((HALVES, n_dev - 1)),
                dma((HALVES, n_dev - 1)),
                dma((n_dev - 1,)),
                dma((n_dev - 1,)),
                dma((CHUNKS, 2, 10)),
                dma((CHUNKS, 2, 10)),
            ],
            compiler_params=pltpu.CompilerParams(
                collective_id=0, has_side_effects=True, vmem_limit_bytes=67_043_328),
            name='fused_head',
        )(hidden, norm_gain, emb_block, teacher_ids, teacher_q)
        grad_block, dh, dw, loss = pl.pallas_call(
            table_kernel,
            in_specs=[any_spec, any_spec, any_spec, vmem_spec, vmem_spec],
            out_specs=(any_spec, any_spec, vmem_spec, vmem_spec),
            out_shape=(
                jax.ShapeDtypeStruct((vocab, dim), F32),
                jax.ShapeDtypeStruct((tokens, dim), BF16),
                jax.ShapeDtypeStruct((dim,), F32),
                jax.ShapeDtypeStruct((1, 128), F32),
            ),
            scratch_shapes=[
                vm((tokens, vocab), BF16),
                vm((tokens, dim), BF16),
                vm((SLOTS, TT, dim), F32),
                vm((tokens, dim), BF16),
                dma((2,)),
                dma((vocab // TT,)),
                dma((SLOTS, 2)),
                dma((2,)),
            ],
            compiler_params=pltpu.CompilerParams(vmem_limit_bytes=67_043_328),
            name='table_grad',
        )(dz, x_in, dh, dw, loss)
        return (loss[0, 0:1], dh, dw, grad_block)

    return jax.shard_map(local_step, mesh=mesh, in_specs=(P('dp', None), P(None), P('tp', None), P('dp', None), P('dp', None)), out_specs=(P('dp'), P('dp', None), P('dp'), P(('dp', 'tp'), None)), check_vma=False)
```
